32 devices in a mesh: dp: 2 (over x), tp: 16 (over z, y, core).
Axes of the slice: x: 2, y: 2, z: 4, core: 2. Of those that a mesh axis runs over, the one named last changes fastest.
Arguments:
- x_in: bfloat16 [6, 2048, 2560], P('dp'), parts along dimension 0
- seq_lens: int32 [6], P('dp'), parts along dimension 0
- ln1_gain: float32 [2560], replicated
- ln1_bias: float32 [2560], replicated
- w_qkv: bfloat16 [2560, 3, 32, 80], P(None, None, 'tp')
- b_qkv: bfloat16 [3, 32, 80], P(None, 'tp')
- w_out: bfloat16 [32, 80, 2560], P('tp')
- b_out: bfloat16 [2560], replicated
- ln2_gain: float32 [2560], replicated
- ln2_bias: float32 [2560], replicated
- w_up: bfloat16 [2560, 10240], P(None, 'tp')
- b_up: bfloat16 [10240], P('tp')
- w_down: bfloat16 [10240, 2560], P('tp')
- b_down: bfloat16 [2560], replicated
Outputs:
- output 1: bfloat16 [6, 2048, 2560], P('dp'), parts along dimension 0
- output 2: bfloat16 [6, 32, 2048, 80], P('dp', 'tp'), parts along dimension 0
- output 3: bfloat16 [6, 32, 2048, 80], P('dp', 'tp'), parts along dimension 0
There are 2 independent parts. The reference program is written for one: setup_inputs(seed, part) draws one part's arguments, and reference() takes and returns one part's arrays. A program takes and returns all parts, laid end to end along the dimension named above; an argument that names none is the same for every part.
All inputs are finite; a program needn't handle non-finite values.
Results may differ from the reference program's by a relative error of at most 0.0137091.
Values are sent between devices in bfloat16 or wider.
A program may use at most 1 GiB of HBM per device.

```python
import jax
import jax.numpy as jnp
from jax import lax

D = 2560
HEADS = 32
HEAD = 80
BATCH = 3
SEQ = 2048
FF = 4 * D
MIN_LEN = SEQ // 8


def setup_inputs(seed: int = 0, part: int = 0) -> dict:
    base_key = jax.random.key(seed)
    weight_keys = jax.random.split(base_key, 12)
    part_key = jax.random.fold_in(base_key, part)
    act_key, len_key = jax.random.split(part_key, 2)
    x_in = jax.random.normal(act_key, (BATCH, SEQ, D), jnp.float32).astype(jnp.bfloat16)
    seq_lens = jax.random.randint(len_key, (BATCH,), MIN_LEN, SEQ, jnp.int32).at[0].set(SEQ)
    return {
        "x_in": x_in,
        "seq_lens": seq_lens,
        "ln1_gain": 1.0 + 0.3 * jax.random.normal(weight_keys[0], (D,), jnp.float32),
        "ln1_bias": 0.3 * jax.random.normal(weight_keys[1], (D,), jnp.float32),
        "w_qkv": (1.5 * D ** -0.5 * jax.random.normal(weight_keys[2], (D, 3, HEADS, HEAD), jnp.float32)).astype(jnp.bfloat16),
        "b_qkv": (0.5 * jax.random.normal(weight_keys[3], (3, HEADS, HEAD), jnp.float32)).astype(jnp.bfloat16),
        "w_out": ((HEADS * HEAD) ** -0.5 * jax.random.normal(weight_keys[4], (HEADS, HEAD, D), jnp.float32)).astype(jnp.bfloat16),
        "b_out": (0.5 * jax.random.normal(weight_keys[5], (D,), jnp.float32)).astype(jnp.bfloat16),
        "ln2_gain": 1.0 + 0.3 * jax.random.normal(weight_keys[6], (D,), jnp.float32),
        "ln2_bias": 0.3 * jax.random.normal(weight_keys[7], (D,), jnp.float32),
        "w_up": (D ** -0.5 * jax.random.normal(weight_keys[8], (D, FF), jnp.float32)).astype(jnp.bfloat16),
        "b_up": (0.5 * jax.random.normal(weight_keys[9], (FF,), jnp.float32)).astype(jnp.bfloat16),
        "w_down": (FF ** -0.5 * jax.random.normal(weight_keys[10], (FF, D), jnp.float32)).astype(jnp.bfloat16),
        "b_down": (0.5 * jax.random.normal(weight_keys[11], (D,), jnp.float32)).astype(jnp.bfloat16),
    }


def layer_norm(values, gain_vec, bias_vec):
    values = values.astype(jnp.float32)
    row_mean = jnp.mean(values, axis=-1, keepdims=True)
    centered = values - row_mean
    row_var = jnp.mean(centered * centered, axis=-1, keepdims=True)
    return (centered * lax.rsqrt(row_var + 1e-5) * gain_vec + bias_vec).astype(jnp.bfloat16)


def cache_keep(values, seq_lens):
    positions = jnp.arange(SEQ)
    valid = positions[None, None, :, None] < seq_lens[:, None, None, None]
    return jnp.where(valid, values, 0)


def attend_one(item):
    q_head, k_head, v_head, length = item
    positions = jnp.arange(SEQ)
    allowed = (positions[None, :] <= positions[:, None]) & (positions[None, :] < length)
    scores = jnp.dot(q_head, k_head.T, preferred_element_type=jnp.float32) * HEAD ** -0.5
    scores = jnp.where(allowed, scores, -1e30)
    attn_probs = jax.nn.softmax(scores, axis=-1).astype(jnp.bfloat16)
    return jnp.dot(attn_probs, v_head, preferred_element_type=jnp.float32).astype(jnp.bfloat16)


def reference(x_in, seq_lens, ln1_gain, ln1_bias, w_qkv, b_qkv, w_out, b_out, ln2_gain, ln2_bias, w_up, b_up, w_down, b_down):
    tok_count = BATCH * SEQ
    inner_width = 3 * HEADS * HEAD
    normed = layer_norm(x_in.reshape(tok_count, D), ln1_gain, ln1_bias)
    qkv_flat = jnp.dot(normed, w_qkv.reshape(D, inner_width), preferred_element_type=jnp.float32)
    qkv_flat = (qkv_flat + b_qkv.reshape(inner_width).astype(jnp.float32)).astype(jnp.bfloat16)
    qkv_all = jnp.transpose(qkv_flat.reshape(BATCH, SEQ, 3, HEADS, HEAD), (2, 0, 3, 1, 4))
    q_all = qkv_all[0]
    k_all = qkv_all[1]
    v_all = qkv_all[2]
    pair_count = BATCH * HEADS
    head_lens = jnp.repeat(seq_lens, HEADS)
    attended = lax.map(attend_one, (q_all.reshape(pair_count, SEQ, HEAD), k_all.reshape(pair_count, SEQ, HEAD), v_all.reshape(pair_count, SEQ, HEAD), head_lens))
    attended = attended.reshape(BATCH, HEADS, SEQ, HEAD)
    out_proj = jnp.einsum("bhsk,hkd->bsd", attended.astype(jnp.float32), w_out.astype(jnp.float32))
    x_mid = (x_in.astype(jnp.float32) + out_proj + b_out.astype(jnp.float32)).astype(jnp.bfloat16)
    normed2 = layer_norm(x_mid.reshape(tok_count, D), ln2_gain, ln2_bias)
    up_proj = jnp.dot(normed2, w_up, preferred_element_type=jnp.float32) + b_up.astype(jnp.float32)
    hidden = jax.nn.relu(up_proj).astype(jnp.bfloat16)
    down_proj = jnp.dot(hidden, w_down, preferred_element_type=jnp.float32) + b_down.astype(jnp.float32)
    x_out = (x_mid.reshape(tok_count, D).astype(jnp.float32) + down_proj).astype(jnp.bfloat16)
    return (x_out.reshape(BATCH, SEQ, D), cache_keep(k_all, seq_lens), cache_keep(v_all, seq_lens))
```

```python
import functools

import jax
import jax.numpy as jnp
from jax import lax
from jax.experimental import pallas as pl
from jax.experimental.pallas import tpu as pltpu
from jax.sharding import PartitionSpec as P

D, S, HD, FF = 2560, 2048, 80, 640
QUART = S // 4
NB, BR, H2, Q4 = 12, 128, 64, 32
MESH = pl.DeviceIdType.MESH
NT = (((1,), (1,)), ((), ()))
TN = (((0,), (0,)), ((), ()))
SCALE = HD ** -0.5
LOG2E = 1.4426950408889634
BF = jnp.bfloat16
ANY = pl.BlockSpec(memory_space=pl.ANY)


def ln_rows(x, gain, bias):
    centered = x - jnp.mean(x, axis=-1, keepdims=True)
    var = jnp.mean(centered * centered, axis=-1, keepdims=True)
    return (centered * lax.rsqrt(var + 1e-5) * gain + bias).astype(jnp.bfloat16)


def qkv_kernel(seq, tb, lens_ref, x_ref, g_ref, b_ref, w_ref, bias_ref, q_ref, k_ref, v_ref):
    h = ln_rows(x_ref[0].astype(jnp.float32), g_ref[...], b_ref[...])
    t = lax.dot_general(w_ref[...], h, NT, preferred_element_type=jnp.float32)
    t = (t + bias_ref[...]).astype(jnp.bfloat16)
    pos = pl.program_id(0) * tb + lax.broadcasted_iota(jnp.int32, (1, tb), 1)
    keep = pos < lens_ref[seq]
    for i in range(2):
        q_ref[i] = t[i * HD:(i + 1) * HD]
        k_ref[i] = jnp.where(keep, t[(2 + i) * HD:(3 + i) * HD], 0)
        v_ref[i] = jnp.where(keep, t[(4 + i) * HD:(5 + i) * HD], 0)


def qkv(seq, lens, x, gain, bias, w, b, tb=512):
    const = lambda shape: pl.BlockSpec(shape, lambda t, *_: (0, 0))
    block = pl.BlockSpec((2, HD, tb), lambda t, *_: (0, 0, t))
    out = jax.ShapeDtypeStruct((2, HD, S), jnp.bfloat16)
    return pl.pallas_call(
        functools.partial(qkv_kernel, seq, tb),
        out_shape=(out, out, out),
        grid_spec=pltpu.PrefetchScalarGridSpec(
            num_scalar_prefetch=1,
            grid=(S // tb,),
            in_specs=[pl.BlockSpec((1, tb, D), lambda t, *_: (seq, t, 0)), const((1, D)), const((1, D)), const((6 * HD, D)), const((6 * HD, 1))],
            out_specs=(block, block, block),
        ),
        cost_estimate=pl.CostEstimate(flops=2 * S * D * 6 * HD, bytes_accessed=2 * S * D, transcendentals=0),
        name="qkv",
    )(lens, x, gain, bias, w, b)


def attn_kernel(seq, qb, lens_ref, half_ref, q_ref, k_ref, v_ref, o_ref, kt):
    i = pl.program_id(0)
    n = lens_ref[seq]

    @pl.when(i == 0)
    def _():
        for h in range(2):
            kt[h] = k_ref[h].T

    nfull = jnp.minimum(i, n // qb)
    key = lax.broadcasted_iota(jnp.int32, (qb, qb), 0)
    rel = key - lax.broadcasted_iota(jnp.int32, (qb, qb), 1)

    def block(h, j, m, l, acc, masked):
        at = pl.ds(pl.multiple_of(j * qb, qb), qb)
        s = jnp.dot(kt[h, at], q_ref[h], preferred_element_type=jnp.float32) * (SCALE * LOG2E)
        if masked:
            s = jnp.where((rel <= (i - j) * qb) & (key < n - j * qb), s, -1e30)
        m_new = jnp.maximum(m, jnp.max(s, axis=0, keepdims=True))
        p = jnp.exp2(s - m_new)
        scale = jnp.exp2(m - m_new)
        l = scale * l + jnp.sum(p, axis=0, keepdims=True)
        acc = scale * acc + jnp.dot(v_ref[h, :, at], p.astype(jnp.bfloat16), preferred_element_type=jnp.float32)
        return m_new, l, acc

    zero = (jnp.full((1, qb), -1e30, jnp.float32), jnp.zeros((1, qb), jnp.float32), jnp.zeros((HD, qb), jnp.float32))
    carry = lax.fori_loop(0, nfull, lambda j, c: tuple(block(h, j, *c[h], False) for h in range(2)), (zero, zero))
    for h in range(2):
        _, l, acc = block(h, nfull, *carry[h], True)
        o_ref[0, 0, h] = (acc / l).astype(jnp.bfloat16)


def attn(seq, lens, place, q, k, v, qb=QUART):
    full = pl.BlockSpec((2, HD, S), lambda t, *_: (0, 0, 0))
    slot = lambda t, lens, place: ((t // 2 + place[1]) % 2, (t + place[2]) % 2, 0, 0, 0)
    return pl.pallas_call(
        functools.partial(attn_kernel, seq, qb),
        out_shape=jax.ShapeDtypeStruct((2, 2, 2, HD, QUART), BF),
        grid_spec=pltpu.PrefetchScalarGridSpec(
            num_scalar_prefetch=2,
            grid=(S // qb,),
            in_specs=[pl.BlockSpec((2, HD, qb), lambda t, *_: (0, 0, t)), full, full],
            out_specs=pl.BlockSpec((1, 1, 2, HD, qb), slot),
            scratch_shapes=[pltpu.VMEM((2, S, HD), BF)],
        ),
        cost_estimate=pl.CostEstimate(flops=4 * S * S * 256, bytes_accessed=2 * S * HD * 8, transcendentals=S * S),
        name="attn",
    )(lens, place, q, k, v)


MASKS = (0, 8, 2, 10, 4, 12, 6, 14, 1, 9, 3, 11, 5, 13, 7, 15)


def mid_kernel(n_seq, place, *refs):
    a_refs, refs = [refs[5 * s:5 * s + 5] for s in range(n_seq)], refs[5 * n_seq:]
    wo_hbm, up_hbm, refs = refs[0], refs[1:12], refs[12:]
    x_ref, bo_ref, g_ref, b_ref, bu_ref, x1_ref, u_ref, wo, wu, a_sc, wsem, usem, asem = refs
    step = pl.program_id(0)
    tb = x_ref.shape[1]
    me, group = place[0], place[3]

    def pieces(s):
        own, z, y, zl, c = a_refs[s]
        return [own.at[0, 0], z.at[0], y.at[0], y.at[1]] + [zl.at[i] for i in range(4)] + [c.at[i] for i in range(8)]

    def a_copies(s):
        return [pltpu.make_async_copy(src, a_sc.at[s, me ^ m], asem.at[s, i]) for i, (src, m) in enumerate(zip(pieces(s), MASKS))]

    def up_copies():
        n = D // 4
        row = lambda g, p: pl.ds(pl.multiple_of(g * 2 * n + p * n, n), n)
        out = [pltpu.make_async_copy(up_hbm[0], wu.at[0], usem.at[0])]
        got, other = group, 1 - group
        plan = [(1, got, 0), (1, got, 1), (1, other, 0), (1, other, 1), (2, got, None), (2, other, None), (3, got, 0), (3, got, 1), (3, other, 0), (3, other, 1)]
        for i, (shard, g, p) in enumerate(plan):
            rows = pl.ds(pl.multiple_of(g * 2 * n, n), 2 * n) if p is None else row(g, p)
            out.append(pltpu.make_async_copy(up_hbm[1 + i], wu.at[shard, rows], usem.at[1 + i]))
        return out

    wo_copy = pltpu.make_async_copy(wo_hbm, wo, wsem)

    @pl.when(step == 0)
    def _():
        for c in a_copies(0):
            c.start()
        wo_copy.start()
        for c in up_copies():
            c.start()
        for s in range(1, n_seq):
            for c in a_copies(s):
                c.start()
        wo_copy.wait()

    per = QUART // tb
    for s in range(n_seq):
        @pl.when(step == s * per)
        def _():
            for c in a_copies(s):
                c.wait()

    seq = step // per
    cols = pl.ds(pl.multiple_of((step % per) * tb, tb), tb)
    a = a_sc[seq, :, :, cols].reshape(D, tb)
    o = lax.dot_general(a, wo[...], TN, preferred_element_type=jnp.float32)
    x1 = (x_ref[0].astype(jnp.float32) + o + bo_ref[...]).astype(BF)
    x1_ref[...] = x1
    h = ln_rows(x1.astype(jnp.float32), g_ref[...], b_ref[...])

    @pl.when(step == 0)
    def _():
        for c in up_copies():
            c.wait()

    for i in range(4):
        at = slice(i * FF, (i + 1) * FF)
        up = jnp.dot(h, wu[i], preferred_element_type=jnp.float32) + bu_ref[:, at]
        u_ref[:, at] = jnp.maximum(up, 0).astype(BF)


def mid(place, a_all, x, wo, ups, bo, gain, bias, bu, tb=256):
    n_seq = x.shape[0]
    const = lambda shape: pl.BlockSpec(shape, lambda t, *_: (0, 0), pipeline_mode=pl.Buffered(1))
    rows = pl.BlockSpec((tb, D), lambda t, *_: (t, 0))
    per = QUART // tb
    out = jax.ShapeDtypeStruct((n_seq * QUART, D), BF)
    flat = [v for seq in a_all for v in seq]
    return pl.pallas_call(
        functools.partial(mid_kernel, n_seq),
        out_shape=(out, out),
        grid_spec=pltpu.PrefetchScalarGridSpec(
            num_scalar_prefetch=1,
            grid=(n_seq * per,),
            in_specs=[ANY] * (len(flat) + 1 + len(ups)) + [
                pl.BlockSpec((1, tb, D), lambda t, place: (t // per, (place[1] * 2 + place[2]) * per + t % per, 0)),
                const((1, D)), const((1, D)), const((1, D)), const((1, 4 * FF)),
            ],
            out_specs=(rows, rows),
            scratch_shapes=[
                pltpu.VMEM((D, D), BF), pltpu.VMEM((4, D, FF), BF), pltpu.VMEM((n_seq, 16, 2 * HD, QUART), BF),
                pltpu.SemaphoreType.DMA, pltpu.SemaphoreType.DMA((11,)), pltpu.SemaphoreType.DMA((n_seq, 16)),
            ],
        ),
        compiler_params=pltpu.CompilerParams(vmem_limit_bytes=60 * 2**20),
        cost_estimate=pl.CostEstimate(flops=4 * n_seq * QUART * D * D, bytes_accessed=4 * D * D, transcendentals=0),
        name="mid",
    )(place, *flat, wo, *ups, x, bo, gain, bias, bu)


def m2_kernel(u_ref, wo_ref, zg, zo, yg, yo, wg, wx, x1_ref, bd_ref, o_ref,
              wd, ub, x1b, part, s1, r1, s2, r2, own, fin,
              wsem, usem, xsem, lsem, s1s, r1s, s2s, r2s, zs, zr, ys, yr, ds, dr):
    dp=lax.axis_index("dp"); tp=lax.axis_index("tp")
    z=tp//4; y=(tp//2)%2; c=tp%2; zl=z%2
    dev=lambda z_,y_,c_: (dp, z_*4+y_*2+c_)
    partner=dev(z,y,1-c); ypeer=dev(z,1-y,c); zpeer=dev(z+1-2*zl,y,c)
    zline=[dev((z+k)%4,y,c) for k in range(4)]
    bar=pltpu.get_barrier_semaphore()
    for t in (partner,ypeer,zline[1],zline[2],zline[3]):
        pl.semaphore_signal(bar,inc=1,device_id=t,device_id_type=MESH)
    loads=[]
    def load(src,dst,sem):
        cp=pltpu.make_async_copy(src,dst,sem); cp.start(); return cp
    n=320
    a=pl.multiple_of(dp*n,n); b_=pl.multiple_of((1-dp)*n,n)
    loads.append(load(wo_ref, wd.at[pl.ds(0,640)], wsem.at[0]))
    for i,(g,o) in enumerate(((zg,zo),(yg,yo),(wg,wx))):
        loads.append(load(g, wd.at[pl.ds(640*(i+1)+a,n)], wsem.at[1+2*i]))
        loads.append(load(o, wd.at[pl.ds(640*(i+1)+b_,n)], wsem.at[2+2*i]))
    rows=lambda b: pl.multiple_of(b*BR,BR)
    def uload(b): return pltpu.make_async_copy(u_ref.at[pl.ds(rows(b),BR)], ub.at[b], usem.at[b])
    off=c*H2+zl*Q4
    def xload(b): return pltpu.make_async_copy(x1_ref.at[pl.ds(pl.multiple_of(b*BR+off,Q4),Q4)], x1b.at[b], xsem.at[b])
    @pl.loop(0,NB)
    def _(b):
        uload(b).start(); xload(b).start()
    for l in loads: l.wait()
    pl.semaphore_wait(bar,5)

    def orows(b,z_,y_,c_):
        seq=b//4; sub=b%4
        pos=512*((z_//2)*2+y_)+BR*sub+c_*H2+(z_%2)*Q4
        return pl.ds(pl.multiple_of(seq*2048+pos,Q4),Q4)
    def send(src,dst,ss,rs,to):
        return pltpu.make_async_remote_copy(src,dst,ss,rs,device_id=to,device_id_type=MESH)
    def rs1(b): return send(s1.at[b],r1.at[b],s1s,r1s.at[b],partner)
    def rs2(b): return send(s2.at[b],r2.at[b],s2s,r2s.at[b],zpeer)
    def agz(b,k):
        return send(fin.at[b], o_ref.at[orows(b,z,y,c)], zs, zr.at[b*4+k], zline[k])
    def agy(b,k):
        r=orows(b,(z-k)%4,y,c)
        return send(fin.at[b] if k==0 else o_ref.at[r], o_ref.at[r], ys, yr.at[b*4+k], ypeer)
    def agd(b,k,yy):
        r=orows(b,(z-k)%4,yy,c)
        return send(fin.at[b] if (k==0 and yy is y) else o_ref.at[r], o_ref.at[r], ds, dr, partner)

    @pl.loop(0,NB+4)
    def _(t):
        @pl.when(t<NB)
        def _():
            uload(t).wait()
            @pl.loop(0,5)
            def _(j):
                cols=pl.ds(pl.multiple_of(j*512,512),512)
                p=jnp.dot(ub[t], wd[:,cols], preferred_element_type=jnp.float32)
                part[t%2,:,cols]=p
            s1[t]=part[t%2,pl.ds(pl.multiple_of((1-c)*H2,H2),H2)].astype(BF)
            rs1(t).start()
        b1=t-1
        @pl.when((b1>=0)&(b1<NB))
        def _():
            rs1(b1).wait_recv()
            other=pl.ds(pl.multiple_of(c*H2+(1-zl)*Q4,Q4),Q4)
            s2[b1]=(part[b1%2,other]+r1[b1,pl.ds(pl.multiple_of((1-zl)*Q4,Q4),Q4)].astype(jnp.float32)).astype(BF)
            rs2(b1).start()
            mine=pl.ds(pl.multiple_of(c*H2+zl*Q4,Q4),Q4)
            own[b1%2]=part[b1%2,mine]+r1[b1,pl.ds(pl.multiple_of(zl*Q4,Q4),Q4)].astype(jnp.float32)
        b2=t-2
        @pl.when((b2>=0)&(b2<NB))
        def _():
            xload(b2).wait()
            rs2(b2).wait_recv()
            down=own[b2%2]+r2[b2].astype(jnp.float32)+bd_ref[...]
            fin[b2]=(x1b[b2].astype(jnp.float32)+down).astype(BF)
            pltpu.make_async_copy(fin.at[b2], o_ref.at[orows(b2,z,y,c)], lsem).start()
            agy(b2,0).start()
            for k in (2,1,3): agz(b2,k).start()
            agd(b2,0,y).start()
        b3=t-3
        @pl.when((b3>=0)&(b3<NB))
        def _():
            for k in (1,3,2):
                agz(b3,k).wait_recv()
                agy(b3,k).start()
                agd(b3,k,y).start()
        b4=t-4
        @pl.when((b4>=0)&(b4<NB))
        def _():
            for k in (0,1,3,2):
                agy(b4,k).wait_recv()
                agd(b4,k,1-y).start()
    def total(sem,ref): pltpu.make_async_copy(ref,ref,sem).wait()
    total(dr, o_ref.at[pl.ds(0,3072)])
    total(ds, o_ref.at[pl.ds(0,3072)])
    total(ys, o_ref.at[pl.ds(0,1536)])
    total(zs, o_ref.at[pl.ds(0,1152)])
    total(lsem, o_ref.at[pl.ds(0,384)])
    total(s1s, s1)
    total(s2s, s2)


def m2(u, wd_own, pieces, x1, bd):
    A=pl.BlockSpec(memory_space=pl.ANY)
    bf=BF
    return pl.pallas_call(m2_kernel, out_shape=jax.ShapeDtypeStruct((6144,D),bf),
        in_specs=[A]*9+[pl.BlockSpec(memory_space=pltpu.VMEM)], out_specs=A,
        scratch_shapes=[pltpu.VMEM((D,D),bf), pltpu.VMEM((NB,BR,D),bf), pltpu.VMEM((NB,Q4,D),bf), pltpu.VMEM((2,BR,D),jnp.float32),
            pltpu.VMEM((NB,H2,D),bf), pltpu.VMEM((NB,H2,D),bf), pltpu.VMEM((NB,Q4,D),bf), pltpu.VMEM((NB,Q4,D),bf), pltpu.VMEM((2,Q4,D),jnp.float32), pltpu.VMEM((NB,Q4,D),bf),
            pltpu.SemaphoreType.DMA((7,)), pltpu.SemaphoreType.DMA((NB,)), pltpu.SemaphoreType.DMA((NB,)), pltpu.SemaphoreType.DMA,
            pltpu.SemaphoreType.DMA, pltpu.SemaphoreType.DMA((NB,)), pltpu.SemaphoreType.DMA, pltpu.SemaphoreType.DMA((NB,)),
            pltpu.SemaphoreType.DMA, pltpu.SemaphoreType.DMA((NB*4,)), pltpu.SemaphoreType.DMA, pltpu.SemaphoreType.DMA((NB*4,)),
            pltpu.SemaphoreType.DMA, pltpu.SemaphoreType.DMA],
        compiler_params=pltpu.CompilerParams(collective_id=0, has_side_effects=True, vmem_limit_bytes=60*2**20),
        cost_estimate=pl.CostEstimate(flops=2*1536*D*D, bytes_accessed=4*D*D, transcendentals=0),
        name="down")(u, wd_own, *pieces, x1, bd)


def solution(mesh):
    tp, dp = mesh.shape["tp"], mesh.shape["dp"]
    both = ("dp", "tp")
    flip = lambda mask: [(d * tp + i, d * tp + (i ^ mask)) for d in range(dp) for i in range(tp)]
    FAR, Y, NEAR, CORE = flip(8), flip(2), flip(4), flip(1)
    PARTNER = [(d * tp + i, (1 - d) * tp + i) for d in range(dp) for i in range(tp)]

    def swap(v, pairs):
        return lax.ppermute(v, both, pairs)

    def local_layer(x_in, seq_lens, ln1_gain, ln1_bias, w_qkv, b_qkv, w_out, b_out, ln2_gain, ln2_bias, w_up, b_up, w_down, b_down):
        group, me = lax.axis_index("dp"), lax.axis_index("tp")
        place = jnp.stack([me, me // 8, (me // 2) % 2, group]).astype(jnp.int32)
        f32 = lambda v: v.astype(jnp.float32).reshape(1, -1)
        n_seq = x_in.shape[0]
        after = lambda v, *deps: lax.optimization_barrier((v, *deps))[0]
        rows = lambda w, start, n: lax.dynamic_slice_in_dim(w, start, n, 0)

        wo = lax.all_gather(w_out.reshape(2 * HD, D), "tp", axis=0, tiled=True)
        bz = swap(b_up, FAR)
        by = swap(jnp.stack([b_up, bz]), Y)
        bu = jnp.concatenate([b_up, bz, by[0], by[1]])
        wq = jnp.transpose(w_qkv, (1, 2, 3, 0)).reshape(6 * HD, D)
        bq = b_qkv.astype(jnp.float32).reshape(6 * HD, 1)
        n = D // 4
        up_half = [rows(w_up, group * 2 * n, n), rows(w_up, group * 2 * n + n, n)]
        up_whole = rows(w_up, group * 2 * n, 2 * n)
        down_half = rows(w_down, group * (FF // 2), FF // 2)
        keys, values = [], []

        def layer(s, gate=None):
            q, k, v = qkv(s, seq_lens if gate is None else after(seq_lens, gate), x_in, f32(ln1_gain), f32(ln1_bias), wq, bq)
            keys.append(k)
            values.append(v)
            return q, k, v

        def attend(s, qkv_s):
            return attn(s, seq_lens, place, *qkv_s).reshape(2, 2, 2 * HD, QUART)

        zu0 = swap(up_half[0], FAR)
        yu = swap(up_whole, Y)
        a0 = attend(0, layer(0))
        z0 = swap(a0[1], FAR)
        zu1 = swap(after(up_half[1], a0), FAR)
        yux = swap(after(yu, a0), PARTNER)
        q1 = layer(1, a0)
        y0 = swap(jnp.stack([a0[0, 1], after(z0, q1[0])[1]]), Y)
        a1 = attend(1, q1)
        z1 = swap(a1[1], FAR)
        zu0 = after(zu0, a1)
        yzu0 = swap(zu0, Y)
        zux0 = swap(zu0, PARTNER)
        y0 = after(y0, a1)
        n0 = swap(jnp.stack([a0[0, 0], z0[0], y0[0], y0[1]]), NEAR)
        q2 = layer(2, a1)
        z1 = after(z1, q2[0])
        y1 = swap(jnp.stack([a1[0, 1], z1[1]]), Y)
        n0 = after(n0, q2[0])
        c0 = swap(jnp.concatenate([jnp.stack([a0[0, 0], z0[0], y0[0], y0[1]]), n0]), CORE)
        a2 = attend(2, q2)
        z2 = swap(a2[1], FAR)
        zu1 = after(zu1, a2)
        yzu1 = swap(zu1, Y)
        zux1 = swap(zu1, PARTNER)
        yzu0 = after(yzu0, a2)
        yzux0 = swap(yzu0, PARTNER)
        y1 = after(y1, a2)
        n1 = swap(jnp.stack([a1[0, 0], z1[0], y1[0], y1[1]]), NEAR)
        zd = swap(after(down_half, a2), FAR)
        yd = swap(after(down_half, a2), Y)
        y2 = swap(jnp.stack([a2[0, 1], z2[1]]), Y)
        yzux1 = swap(yzu1, PARTNER)
        n2 = swap(jnp.stack([a2[0, 0], z2[0], y2[0], y2[1]]), NEAR)
        c1 = swap(jnp.concatenate([jnp.stack([a1[0, 0], z1[0], y1[0], y1[1]]), n1]), CORE)
        c2 = swap(jnp.concatenate([jnp.stack([a2[0, 0], z2[0], y2[0], y2[1]]), n2]), CORE)
        ydx = swap(yd, PARTNER)
        a_all = [(a0, z0, y0, n0, c0), (a1, z1, y1, n1, c1), (a2, z2, y2, n2, c2)]
        ups = [w_up, zu0, zu1, zux0, zux1, yu, yux, yzu0, yzu1, yzux0, yzux1]
        x1, u = mid(place, a_all, x_in, wo, ups, f32(b_out), f32(ln2_gain), f32(ln2_bias), f32(bu))
        zd = after(zd, u) if MID_BEFORE_ZD else zd
        yzd = swap(zd, Y)
        zdx = swap(zd, PARTNER)
        yzdx = swap(yzd, PARTNER)
        x_out = m2(u, w_down, (zd, zdx, yd, ydx, yzd, yzdx), x1, f32(b_down)).reshape(n_seq, S, D)
        cache = lambda c: jnp.swapaxes(jnp.stack(c), 2, 3)
        return x_out, cache(keys), cache(values)

    arg_specs = (P("dp", None, None), P("dp"), P(), P(), P(None, None, "tp", None), P(None, "tp", None), P("tp", None, None), P(), P(), P(), P(None, "tp"), P("tp"), P("tp", None), P())
    cache_spec = P("dp", "tp", None, None)
    return jax.shard_map(local_layer, mesh=mesh, in_specs=arg_specs, out_specs=(P("dp", None, None), cache_spec, cache_spec), check_vma=False)


MID_BEFORE_ZD = False
```

```python
import functools

import jax
import jax.numpy as jnp
from jax import lax
from jax.experimental import pallas as pl
from jax.experimental.pallas import tpu as pltpu
from jax.sharding import PartitionSpec as P

D, S, HD, FF = 2560, 2048, 80, 640
BF = jnp.bfloat16
MESH = pl.DeviceIdType.MESH
ANY = pl.BlockSpec(memory_space=pl.ANY)
NT = (((1,), (1,)), ((), ()))
TN = (((0,), (0,)), ((), ()))
SCALE = HD ** -0.5
LOG2E = 1.4426950408889634


def ln_rows(x, gain, bias):
    centered = x - jnp.mean(x, axis=-1, keepdims=True)
    var = jnp.mean(centered * centered, axis=-1, keepdims=True)
    return (centered * lax.rsqrt(var + 1e-5) * gain + bias).astype(BF)


TB, KA, NS = 256, 96, 3
QB = S // 4
PER_SEQ = S // TB
UC = 2
CHUNKS = tuple((s, h) for s in range(NS) for h in range(2))


def front_kernel(lens_ref, x_ref, vec_ref, wq_ref, bq_ref, wo_ref, wup_ref, bup_ref, wdn_ref,
                 k_out, v_out, x1_out, u_out, dn_out,
                 wt, wu, a_all, xb, q_s, k_s, v_s, kt, a_st, bu, st1, st2,
                 xsem, csem, osem, lsem, wsem, wos, wor, wol, woy_s, woy_r, wod_s, wod_r, ay_s, ay_r, as_, ar, al, ad_s, ad_r,
                 b_s, b_r, yu_s, yu_r, yd_s, yd_r, xu_s, xu_r, xd_s, xd_r):
    group, me = lax.axis_index("dp"), lax.axis_index("tp")
    z, y, c = me // 4, (me // 2) % 2, me % 2
    dev = lambda z_, y_, c_: (group, z_ * 4 + y_ * 2 + c_)
    partner, ypeer, across = dev(z, y, 1 - c), dev(z, 1 - y, c), (1 - group, me)
    right, left = dev((z + 1) % 4, y, c), dev((z + 3) % 4, y, c)
    ln1_gain, ln1_bias, b_out, ln2_gain, ln2_bias = (vec_ref[i:i + 1] for i in range(5))
    sent = []

    def remote(src, dst, ss, rs, to):
        return pltpu.make_async_remote_copy(src, dst, ss, rs, device_id=to, device_id_type=MESH)

    def go(copy, when=None):
        if when is None:
            copy.start()
        else:
            @pl.when(when)
            def _():
                copy.start()
        sent.append((copy, when))

    place = lambda z_, y_, c_: (z_ * 2 + c_) * 2 + y_
    mine = place(z, y, c)
    wo_rows = lambda z_, y_: wt.at[pl.ds(pl.multiple_of(place(z_, y_, c) * 2 * HD, 32), 2 * HD)]

    def wo_line(k, to_right):
        z_ = (z + 4 - k) % 4 if to_right else (z + k) % 4
        rows = wo_rows(z_, y)
        i = k + 3 * (not to_right)
        return remote(wo_ref if k == 0 else rows, rows, wos.at[i], (wor if to_right else wol).at[k], right if to_right else left)

    def wo_y(z_, own=False):
        rows = wo_rows(z_, y)
        return remote(wo_ref if own else rows, rows, woy_s.at[z_], woy_r.at[z_], ypeer)

    def wo_core(z_, y_, own=False):
        rows = wo_rows(z_, y_)
        return remote(wo_ref if own else rows, rows, wod_s, wod_r, partner)

    def a_y(i):
        s, h = CHUNKS[i]
        return remote(a_st.at[s, 2 * (1 - y) + h], a_all.at[s, h, mine], ay_s.at[i], ay_r.at[i], ypeer)

    def a_line(i, k, to_right):
        s, h = CHUNKS[i]
        z_ = (z + 4 - k) % 4 if to_right else (z + k) % 4
        pair = a_all.at[s, h, pl.ds(place(z_, 0, c), 2)]
        return remote(pair, pair, as_.at[i * 6 + k + 3 * (not to_right)], (ar if to_right else al).at[i * 3 + k], right if to_right else left)

    def a_core(i, z_):
        s, h = CHUNKS[i]
        pair = a_all.at[s, h, pl.ds(place(z_, 0, c), 2)]
        return remote(pair, pair, ad_s.at[i], ad_r.at[i], partner)

    hu, hd = D // 2, FF // 2
    cu, cd = hu // UC, hd // UC

    def up_rows(n):
        return pl.ds(pl.multiple_of(group * hu + n * cu, 32), cu)

    def dn_rows(n):
        return pl.ds(pl.multiple_of(group * hd + n * cd, 32), cd)

    def yu(n):
        return remote(wup_ref.at[up_rows(n)], wu.at[1, up_rows(n)], yu_s.at[n], yu_r.at[n], ypeer)

    def xu(n):
        return remote(wu.at[1, up_rows(n)], wu.at[1, up_rows(n)], xu_s.at[n], xu_r.at[n], across)

    def yd(n):
        return remote(wdn_ref.at[dn_rows(n)], dn_out.at[dn_rows(n)], yd_s.at[n], yd_r.at[n], ypeer)

    def xd(n):
        return remote(dn_out.at[dn_rows(n)], dn_out.at[dn_rows(n)], xd_s.at[n], xd_r.at[n], across)

    bias_flow = remote(bup_ref, bu.at[1], b_s, b_r, ypeer)

    def hop(line, k, then):
        @pl.when(z >= k + 1)
        def _():
            line(k, True).wait_recv()

        if k < 2:
            go(line(k + 1, True), (z >= k + 1) & (z < 3))
        then((z + 3 - k) % 4, z >= k + 1)

        @pl.when(z <= 2 - k)
        def _():
            line(k, False).wait_recv()

        if k < 2:
            go(line(k + 1, False), (z <= 2 - k) & (z > 0))
        then((z + 1 + k) % 4, z <= 2 - k)

    def begin(line):
        go(line(0, True), z < 3)
        go(line(0, False), z > 0)

    def start_if(copy, when):
        @pl.when(when)
        def _():
            copy.start()

    def wo_then(z_, when):
        start_if(wo_y(z_), when)
        start_if(wo_core(z_, y), when)

    def wo_hop(k):
        hop(wo_line, k, wo_then)

    def wo_from_y():
        for z_ in range(4):
            wo_y(z_).wait_recv()
            wo_core(z_, 1 - y).start()

    def a_begin(s):
        for i in (2 * s, 2 * s + 1):
            a_y(i).wait_recv()
            begin(functools.partial(a_line, i))
            a_core(i, z).start()

    def a_hop(s, k):
        for i in (2 * s, 2 * s + 1):
            hop(functools.partial(a_line, i), k, lambda z_, when: start_if(a_core(i, z_), when))

    barrier = pltpu.get_barrier_semaphore()
    peers = (partner, ypeer, across, right, left)
    for p in peers:
        pl.semaphore_signal(barrier, inc=1, device_id=p, device_id_type=MESH)

    def x_copy(g):
        return pltpu.make_async_copy(x_ref.at[g // PER_SEQ, pl.ds(pl.multiple_of((g % PER_SEQ) * TB, TB), TB)], xb.at[g % 2], xsem.at[g % 2])

    x_copy(0).start()
    locals_ = [pltpu.make_async_copy(wo_ref, wo_rows(z, y), wsem.at[0]), pltpu.make_async_copy(bup_ref, bu.at[0], wsem.at[1]), pltpu.make_async_copy(wup_ref, wu.at[0], wsem.at[2])]
    for copy in locals_:
        copy.start()
    row = lax.broadcasted_iota(jnp.int32, (KA - HD, S), 0)
    for h in range(2):
        q_s[h, HD:] = jnp.where(row == 0, 1.0, 0.0).astype(BF)
    pl.semaphore_wait(barrier, len(peers))

    begin(wo_line)
    wo_y(z, True).start()
    wo_core(z, y, True).start()
    go(bias_flow)

    def qkv(s):
        n = lens_ref[s]

        @pl.loop(0, PER_SEQ)
        def _(b):
            g = s * PER_SEQ + b
            x_copy(g).wait()

            @pl.when(g + 1 < NS * PER_SEQ)
            def _():
                x_copy(g + 1).start()

            h = ln_rows(xb[g % 2].astype(jnp.float32), ln1_gain, ln1_bias)
            t = lax.dot_general(wq_ref[...], h, NT, preferred_element_type=jnp.float32)
            t = (t + bq_ref[...]).astype(BF)
            cols = pl.ds(pl.multiple_of(b * TB, TB), TB)
            keep = b * TB + lax.broadcasted_iota(jnp.int32, (1, TB), 1) < n
            for i in range(2):
                q_s[i, :HD, cols] = t[i * HD:(i + 1) * HD]
                k_s[i, :HD, cols] = jnp.where(keep, t[(2 + i) * HD:(3 + i) * HD], 0)
                v_s[i, :, cols] = jnp.where(keep, t[(4 + i) * HD:(5 + i) * HD], 0)

        pos = lax.broadcasted_iota(jnp.int32, (KA - HD, S), 1)
        for i in range(2):
            k_s[i, HD:] = jnp.where((row == 0) & (pos >= n), -1e30, 0.0).astype(BF)
            kt[i] = k_s[i].T
        for copy in caches(s):
            copy.start()

    def caches(s):
        return [pltpu.make_async_copy(k_s.at[:, pl.ds(0, HD)], k_out.at[s], csem.at[0]), pltpu.make_async_copy(v_s, v_out.at[s], csem.at[1])]

    def attend(s):
        causal = lax.broadcasted_iota(jnp.int32, (QB, QB), 0) <= lax.broadcasted_iota(jnp.int32, (QB, QB), 1)

        @pl.loop(0, 4)
        def _(t):
            at_q = pl.ds(pl.multiple_of(t * QB, QB), QB)

            def block(h, j, m, l, acc, masked):
                at = pl.ds(pl.multiple_of(j * QB, QB), QB)
                sc = jnp.dot(kt[h, at], q_s[h, :, at_q], preferred_element_type=jnp.float32) * (SCALE * LOG2E)
                if masked:
                    sc = jnp.where(causal, sc, -1e30)
                m_new = jnp.maximum(m, jnp.max(sc, axis=0, keepdims=True))
                p = jnp.exp2(sc - m_new)
                scale = jnp.exp2(m - m_new)
                l = scale * l + jnp.sum(p, axis=0, keepdims=True)
                acc = scale * acc + jnp.dot(v_s[h, :, at], p.astype(BF), preferred_element_type=jnp.float32)
                return m_new, l, acc

            zero = (jnp.full((1, QB), -1e30, jnp.float32), jnp.zeros((1, QB), jnp.float32), jnp.zeros((HD, QB), jnp.float32))
            carry = lax.fori_loop(0, t, lambda j, c: tuple(block(h, j, *c[h], False) for h in range(2)), (zero, zero))
            for h in range(2):
                _, l, acc = block(h, t, *carry[h], True)
                a_st[s, t, h * HD:(h + 1) * HD] = (acc / l).astype(BF)

            @pl.when(t // 2 == y)
            def _():
                a_all[s, t % 2, mine] = a_st[s, t]

        for copy in caches(s):
            copy.wait()
        go(a_y(2 * s))
        go(a_y(2 * s + 1))

    per = QB // TB
    n_blocks = NS * 2 * per

    def res_copy(i):
        rows = pl.ds(pl.multiple_of(y * (S // 2) + (i % (2 * per)) * TB, TB), TB)
        return pltpu.make_async_copy(x_ref.at[i // (2 * per), rows], xb.at[i % 2], xsem.at[i % 2])

    def put_x1(i):
        return pltpu.make_async_copy(st1.at[i % 2], x1_out.at[pl.ds(pl.multiple_of(i * TB, TB), TB)], osem.at[i % 2])

    def put_u(i):
        return pltpu.make_async_copy(st2.at[i % 2], u_out.at[pl.ds(pl.multiple_of(i * TB, TB), TB)], lsem.at[i % 2])

    def middle(i):
        s, h = CHUNKS[i]
        whole = a_all.at[s, h, pl.ds(0, 8)]
        pltpu.make_async_copy(whole, whole, ad_r.at[i]).wait()

        @pl.loop(i * per, (i + 1) * per)
        def _(b):
            res_copy(b).wait()

            @pl.when(b + 1 < n_blocks)
            def _():
                res_copy(b + 1).start()

            a = a_all[s, h, :, :, pl.ds(pl.multiple_of((b % per) * TB, TB), TB)].reshape(D, TB)
            o = lax.dot_general(a, wt[...], TN, preferred_element_type=jnp.float32)
            x1 = (xb[b % 2].astype(jnp.float32) + o + b_out).astype(BF)

            @pl.when(b >= 2)
            def _():
                put_x1(b - 2).wait()
                put_u(b - 2).wait()

            st1[b % 2] = x1
            put_x1(b).start()
            hid = ln_rows(x1.astype(jnp.float32), ln2_gain, ln2_bias)
            for n in range(2):
                up = jnp.dot(hid, wu[n], preferred_element_type=jnp.float32) + bu[n, 0:1]
                st2[b % 2, :, n * FF:(n + 1) * FF] = jnp.maximum(up, 0).astype(BF)
            put_u(b).start()

    qkv(0)
    wo_hop(0)
    attend(0)
    wo_hop(1)
    go(yu(0))
    qkv(1)
    a_begin(0)
    wo_hop(2)
    attend(1)
    go(yu(1))
    a_hop(0, 0)
    wo_from_y()
    qkv(2)
    a_hop(0, 1)
    a_begin(1)
    attend(2)
    res_copy(0).start()
    for n in range(UC):
        go(yd(n))
    for n in range(UC):
        yu(n).wait_recv()
        go(xu(n))
    a_hop(0, 2)
    a_hop(1, 0)
    whole = wt.at[pl.ds(0, D // 2)]
    pltpu.make_async_copy(whole, whole, wod_r).wait()
    bias_flow.wait_recv()
    for copy in locals_:
        copy.wait()
    a_begin(2)
    a_hop(1, 1)
    for n in range(UC):
        xu(n).wait_recv()
    middle(0)
    a_hop(2, 0)
    a_hop(1, 2)
    for n in range(UC):
        yd(n).wait_recv()
        go(xd(n))
    middle(1)
    a_hop(2, 1)
    middle(2)
    a_hop(2, 2)
    middle(3)
    middle(4)
    middle(5)
    for n in range(UC):
        xd(n).wait_recv()
    for b in range(n_blocks - 2, n_blocks):
        put_x1(b).wait()
        put_u(b).wait()
    for copy, when in sent:
        if when is None:
            copy.wait_send()
        else:
            @pl.when(when)
            def _():
                copy.wait_send()
    for z_ in range(4):
        wo_y(z_).wait_send()
    pltpu.make_async_copy(whole, whole, wod_s).wait()
    for i, (s, h) in enumerate(CHUNKS):
        pairs = a_all.at[s, h, pl.ds(0, 8)]
        pltpu.make_async_copy(pairs, pairs, ad_s.at[i]).wait()


def front(lens, x, vec, wq, bq, wo, wup, bup, wdn):
    v = pl.BlockSpec(memory_space=pltpu.VMEM)
    sem = lambda n: pltpu.SemaphoreType.DMA((n,))
    one = pltpu.SemaphoreType.DMA
    cache = jax.ShapeDtypeStruct((NS, 2, HD, S), BF)
    rows = lambda n: jax.ShapeDtypeStruct((NS * S // 2, n), BF)
    nc = len(CHUNKS)
    return pl.pallas_call(
        front_kernel,
        out_shape=(cache, cache, rows(D), rows(2 * FF), jax.ShapeDtypeStruct((FF, D), BF)),
        in_specs=[pl.BlockSpec(memory_space=pltpu.SMEM), ANY, v, v, v, ANY, ANY, ANY, ANY],
        out_specs=(ANY,) * 5,
        scratch_shapes=[
            pltpu.VMEM((D, D), BF), pltpu.VMEM((2, D, FF), BF), pltpu.VMEM((NS, 2, 16, 2 * HD, QB), BF), pltpu.VMEM((2, TB, D), BF),
            pltpu.VMEM((2, KA, S), BF), pltpu.VMEM((2, KA, S), BF), pltpu.VMEM((2, HD, S), BF), pltpu.VMEM((2, S, KA), BF),
            pltpu.VMEM((NS, 4, 2 * HD, QB), BF), pltpu.VMEM((2, 8, FF), jnp.float32), pltpu.VMEM((2, TB, D), BF), pltpu.VMEM((2, TB, 2 * FF), BF),
            sem(2), sem(2), sem(2), sem(2), sem(3), sem(6), sem(3), sem(3), sem(4), sem(4), one, one, sem(nc), sem(nc), sem(6 * nc), sem(3 * nc), sem(3 * nc), sem(nc), sem(nc),
            one, one, sem(UC), sem(UC), sem(UC), sem(UC), sem(UC), sem(UC), sem(UC), sem(UC),
        ],
        compiler_params=pltpu.CompilerParams(collective_id=1, has_side_effects=True, vmem_limit_bytes=63 * 2**20),
        cost_estimate=pl.CostEstimate(flops=10**11, bytes_accessed=10**8, transcendentals=0),
        name="front",
    )(lens, x, vec, wq, bq, wo, wup, bup, wdn)


BR = 128
NB = 3 * S // 2 // BR
Q = BR // 8
CH = BR // 2
SLOTS, S1N = 6, 4


def down_kernel(u_ref, w0_ref, w1_ref, x1_ref, bd_ref, o_ref,
                wd, ub, x1b, pt, acc, s1, r1, sm, rr, rl, fin,
                wsem, usem, xsem, lsem, s1s, r1s, sms, rrs, rls, zs, frs, fls, ys, yr, ds, dr):
    group, me = lax.axis_index("dp"), lax.axis_index("tp")
    z, y, c = me // 4, (me // 2) % 2, me % 2
    dev = lambda z_, y_, c_: (group, z_ * 4 + y_ * 2 + c_)
    partner, ypeer = dev(z, y, 1 - c), dev(z, 1 - y, c)
    right, left = dev((z + 1) % 4, y, c), dev((z + 3) % 4, y, c)

    barrier = pltpu.get_barrier_semaphore()
    for peer in (partner, ypeer, right, left):
        pl.semaphore_signal(barrier, inc=1, device_id=peer, device_id_type=MESH)

    loads = [pltpu.make_async_copy(w, wd.at[pl.ds(i * FF, FF)], wsem.at[i]) for i, w in enumerate((w0_ref, w1_ref))]
    for copy in loads:
        copy.start()

    def u_load(b):
        return pltpu.make_async_copy(u_ref.at[pl.ds(pl.multiple_of(b * BR, BR), BR)], ub.at[b], usem.at[b])

    def x1_load(b):
        rows = pl.ds(pl.multiple_of(b * BR + c * CH + z * Q, Q), Q)
        return pltpu.make_async_copy(x1_ref.at[rows], x1b.at[b], xsem.at[b])

    @pl.loop(0, NB)
    def _(b):
        u_load(b).start()
        x1_load(b).start()

    for copy in loads:
        copy.wait()
    pl.semaphore_wait(barrier, 4)

    per = NB // 3

    def rows_of(b, z_, y_):
        pos = (S // 2) * y_ + BR * (b % per) + CH * c + Q * z_
        return pl.ds(pl.multiple_of((b // per) * S + pos, Q), Q)

    def remote(src, dst, ss, rs, to):
        return pltpu.make_async_remote_copy(src, dst, ss, rs, device_id=to, device_id_type=MESH)

    def swap(b):
        return remote(s1.at[b % S1N], r1.at[b], s1s.at[b % S1N], r1s.at[b], partner)

    def chain(b, n, at, to_right):
        dst, sem = (rr, rrs) if to_right else (rl, rls)
        return remote(sm.at[b, pl.ds(at, n * Q)], dst.at[b, pl.ds(0, n * Q)], sms, sem.at[b], right if to_right else left)

    def go_right(b, k):
        rows = rows_of(b, (z + 4 - k) % 4, y)
        return remote(fin.at[b] if k == 0 else o_ref.at[rows], o_ref.at[rows], zs, frs.at[b * 3 + k], right)

    def go_left(b, k):
        rows = rows_of(b, (z + k) % 4, y)
        return remote(fin.at[b] if k == 0 else o_ref.at[rows], o_ref.at[rows], zs, fls.at[b * 3 + k], left)

    def go_y(b, z_, own=False):
        rows = rows_of(b, z_, y)
        return remote(fin.at[b] if own else o_ref.at[rows], o_ref.at[rows], ys, yr.at[b * 4 + z_], ypeer)

    def go_core(b, z_, y_, own=False):
        rows = rows_of(b, z_, y_)
        return remote(fin.at[b] if own else o_ref.at[rows], o_ref.at[rows], ds, dr, partner)

    f32 = lambda v: v.astype(jnp.float32)

    def multiply(b):
        u_load(b).wait()

        @pl.when(b >= S1N)
        def _():
            swap(b - S1N).wait_send()

        @pl.loop(0, 5)
        def _(j):
            cols = pl.ds(pl.multiple_of(j * 512, 512), 512)
            pt[...] = jnp.dot(ub[b], wd[:, cols], preferred_element_type=jnp.float32)
            acc[b % SLOTS, :, cols] = pt[pl.ds(pl.multiple_of(c * CH, CH), CH)]
            s1[b % S1N, :, cols] = pt[pl.ds(pl.multiple_of((1 - c) * CH, CH), CH)].astype(BF)

        swap(b).start()

    def own(i, n=1):
        return slice(i * Q, (i + n) * Q)

    def stage2(b):
        swap(b).wait_recv()
        acc[b % SLOTS] += f32(r1[b])

        @pl.when(z == 0)
        def _():
            sm[b] = acc[b % SLOTS, own(1, 3)].astype(BF)
            chain(b, 3, 0, True).start()

        @pl.when(z == 3)
        def _():
            sm[b] = acc[b % SLOTS, own(0, 3)].astype(BF)
            chain(b, 3, 0, False).start()

    def stage3(b):
        a = acc.at[b % SLOTS]

        @pl.when(z == 1)
        def _():
            chain(b, 3, 0, True).wait_recv()
            a[own(1)] += f32(rr[b, own(0)])
            sm[b, own(0, 2)] = (a[own(2, 2)] + f32(rr[b, own(1, 2)])).astype(BF)
            chain(b, 2, 0, True).start()

        @pl.when(z == 2)
        def _():
            chain(b, 3, 0, False).wait_recv()
            a[own(2)] += f32(rl[b, own(2)])
            sm[b, own(0, 2)] = (a[own(0, 2)] + f32(rl[b, own(0, 2)])).astype(BF)
            chain(b, 2, 0, False).start()

    def stage4(b):
        a = acc.at[b % SLOTS]

        @pl.when(z == 2)
        def _():
            chain(b, 2, 0, True).wait_recv()
            a[own(2)] += f32(rr[b, own(0)])
            sm[b, own(2)] = (a[own(3)] + f32(rr[b, own(1)])).astype(BF)
            chain(b, 1, 2 * Q, True).start()

        @pl.when(z == 1)
        def _():
            chain(b, 2, 0, False).wait_recv()
            a[own(1)] += f32(rl[b, own(1)])
            sm[b, own(2)] = (a[own(0)] + f32(rl[b, own(0)])).astype(BF)
            chain(b, 1, 2 * Q, False).start()

    def finish(b):
        a = acc.at[b % SLOTS]

        @pl.when(z == 3)
        def _():
            chain(b, 1, 2 * Q, True).wait_recv()
            a[own(3)] += f32(rr[b, own(0)])

        @pl.when(z == 0)
        def _():
            chain(b, 1, 2 * Q, False).wait_recv()
            a[own(0)] += f32(rl[b, own(0)])

        x1_load(b).wait()
        down = a[pl.ds(pl.multiple_of(z * Q, Q), Q)] + bd_ref[...]
        fin[b] = (f32(x1b[b]) + down).astype(BF)
        go_y(b, z, True).start()

        @pl.when(z < 3)
        def _():
            go_right(b, 0).start()

        @pl.when(z > 0)
        def _():
            go_left(b, 0).start()

        go_core(b, z, y, True).start()
        pltpu.make_async_copy(fin.at[b], o_ref.at[rows_of(b, z, y)], lsem).start()

    def relay(b, k):
        @pl.when(z >= k + 1)
        def _():
            go_right(b, k).wait_recv()
            if k < 2:
                @pl.when(z < 3)
                def _():
                    go_right(b, k + 1).start()
            go_y(b, (z + 3 - k) % 4).start()
            go_core(b, (z + 3 - k) % 4, y).start()

        @pl.when(z <= 2 - k)
        def _():
            go_left(b, k).wait_recv()
            if k < 2:
                @pl.when(z > 0)
                def _():
                    go_left(b, k + 1).start()
            go_y(b, (z + 1 + k) % 4).start()
            go_core(b, (z + 1 + k) % 4, y).start()

    def across(b):
        for z_ in range(4):
            go_y(b, z_).wait_recv()
            go_core(b, z_, 1 - y).start()

    stages = (multiply, stage2, stage3, stage4, finish, functools.partial(relay, k=0), functools.partial(relay, k=1), functools.partial(relay, k=2), across)

    @pl.loop(0, NB + len(stages) - 1)
    def _(t):
        for i, stage in enumerate(stages):
            b = t - i

            @pl.when((b >= 0) & (b < NB))
            def _():
                stage(b)

    def drain(sem, n):
        rows = o_ref.at[pl.ds(0, n)]
        pltpu.make_async_copy(rows, rows, sem).wait()

    n = NB * Q
    drain(dr, 8 * n)
    drain(ds, 8 * n)
    drain(ys, 4 * n)
    drain(lsem, n)
    drain(sms, 3 * n)
    ends = (z == 0) | (z == 3)

    @pl.when(ends)
    def _():
        drain(zs, n)

    @pl.when(jnp.logical_not(ends))
    def _():
        drain(zs, 5 * n)

    for b in range(NB - S1N, NB):
        swap(b).wait_send()


def down(u, w0, w1, x1, bd):
    sem = lambda n: pltpu.SemaphoreType.DMA((n,))
    one = pltpu.SemaphoreType.DMA
    return pl.pallas_call(
        down_kernel,
        out_shape=jax.ShapeDtypeStruct((3 * S, D), BF),
        in_specs=[ANY] * 4 + [pl.BlockSpec(memory_space=pltpu.VMEM)],
        out_specs=ANY,
        scratch_shapes=[
            pltpu.VMEM((2 * FF, D), BF), pltpu.VMEM((NB, BR, 2 * FF), BF), pltpu.VMEM((NB, Q, D), BF), pltpu.VMEM((BR, 512), jnp.float32),
            pltpu.VMEM((SLOTS, CH, D), jnp.float32), pltpu.VMEM((S1N, CH, D), BF), pltpu.VMEM((NB, CH, D), BF),
            pltpu.VMEM((NB, 3 * Q, D), BF), pltpu.VMEM((NB, 3 * Q, D), BF), pltpu.VMEM((NB, 3 * Q, D), BF), pltpu.VMEM((NB, Q, D), BF),
            sem(2), sem(NB), sem(NB), one, sem(S1N), sem(NB), one, sem(NB), sem(NB), one, sem(3 * NB), sem(3 * NB), one, sem(4 * NB), one, one,
        ],
        compiler_params=pltpu.CompilerParams(collective_id=0, has_side_effects=True, vmem_limit_bytes=62 * 2**20),
        cost_estimate=pl.CostEstimate(flops=4 * S * D * D, bytes_accessed=4 * D * D, transcendentals=0),
        name="down",
    )(u, w0, w1, x1, bd)


def solution(mesh):
    def local_layer(x_in, seq_lens, ln1_gain, ln1_bias, w_qkv, b_qkv, w_out, b_out, ln2_gain, ln2_bias, w_up, b_up, w_down, b_down):
        f32 = lambda v: v.astype(jnp.float32)
        wq = jnp.transpose(w_qkv, (1, 2, 3, 0)).reshape(6 * HD, D)
        bq = f32(b_qkv).reshape(6 * HD, 1)
        vec = jnp.stack([ln1_gain, ln1_bias, f32(b_out), ln2_gain, ln2_bias, f32(b_down)])
        bup = jnp.broadcast_to(f32(b_up)[None], (8, FF))
        keys, values, x1, u, down_y = front(seq_lens, x_in, vec, wq, bq, w_out.reshape(2 * HD, D), w_up, bup, w_down)
        x_out = down(u, w_down, down_y, x1, vec[5:6]).reshape(x_in.shape)
        return x_out, jnp.swapaxes(keys, 2, 3), jnp.swapaxes(values, 2, 3)

    arg_specs = (P("dp", None, None), P("dp"), P(), P(), P(None, None, "tp", None), P(None, "tp", None), P("tp", None, None), P(), P(), P(), P(None, "tp"), P("tp"), P("tp", None), P())
    cache_spec = P("dp", "tp", None, None)
    return jax.shard_map(local_layer, mesh=mesh, in_specs=arg_specs, out_specs=(P("dp", None, None), cache_spec, cache_spec), check_vma=False)
```

```python
import functools

import jax
import jax.numpy as jnp
from jax import lax
from jax.experimental import pallas as pl
from jax.experimental.pallas import tpu as pltpu
from jax.sharding import PartitionSpec as P

D, S, HD, FF = 2560, 2048, 80, 640
BF = jnp.bfloat16
MESH = pl.DeviceIdType.MESH
ANY = pl.BlockSpec(memory_space=pl.ANY)
NT = (((1,), (1,)), ((), ()))
TN = (((0,), (0,)), ((), ()))
SCALE = HD ** -0.5
LOG2E = 1.4426950408889634


def ln_rows(x, gain, bias):
    centered = x - jnp.mean(x, axis=-1, keepdims=True)
    var = jnp.mean(centered * centered, axis=-1, keepdims=True)
    return (centered * lax.rsqrt(var + 1e-5) * gain + bias).astype(BF)


TB, KA, NS = 256, 96, 3
QB = S // 4
PER_SEQ = S // TB
UC = 4
LAG = 4
RING = LAG + 1
CHUNKS = tuple((s, h) for s in range(NS) for h in range(2))


def front_kernel(lens_ref, x_ref, vec_ref, wq_ref, bq_ref, wo_ref, wup_ref, bup_ref, wdn_ref,
                 k_out, v_out, x1_out, u_out, dn_out,
                 wt, wu, a_all, xb, q_s, k_s, v_s, kt, a_st, bu, st1, st2, hid,
                 xsem, csem, osem, lsem, wsem, wos, wor, wol, woy_s, woy_r, wox_s, wox_r, wod_s, wod_r, ay_s, ay_r, as_, ar, al, ad_s, ad_r,
                 b_s, b_r, yu_s, yu_r, yd_s, yd_r, xu_s, xu_r, xd_s, xd_r):
    group, me = lax.axis_index("dp"), lax.axis_index("tp")
    z, y, c = me // 4, (me // 2) % 2, me % 2
    dev = lambda z_, y_, c_: (group, z_ * 4 + y_ * 2 + c_)
    partner, ypeer, across = dev(z, y, 1 - c), dev(z, 1 - y, c), (1 - group, me)
    right, left = dev((z + 1) % 4, y, c), dev((z + 3) % 4, y, c)
    ln1_gain, ln1_bias, b_out, ln2_gain, ln2_bias = (vec_ref[i:i + 1] for i in range(5))
    sent = []

    def remote(src, dst, ss, rs, to):
        return pltpu.make_async_remote_copy(src, dst, ss, rs, device_id=to, device_id_type=MESH)

    def go(make, when=None):
        if when is None:
            make().start()
        else:
            @pl.when(when())
            def _():
                make().start()
        sent.append((make, when))

    place = lambda z_, y_, c_: (z_ * 2 + c_) * 2 + y_
    mine = place(z, y, c)
    half = HD

    def wo_part(z_, y_):
        return wt.at[pl.ds(pl.multiple_of(place(z_, y_, c) * 2 * HD + group * half, 16), half)]

    def wo_whole(z_, y_):
        return wt.at[pl.ds(pl.multiple_of(place(z_, y_, c) * 2 * HD, 32), 2 * HD)]

    def wo_mine():
        return wo_ref.at[pl.ds(pl.multiple_of(group * half, 16), half)]

    def wo_line(k, to_right):
        z_ = (z + 4 - k) % 4 if to_right else (z + k) % 4
        i = k + 3 * (not to_right)
        return remote(wo_mine() if k == 0 else wo_part(z_, y), wo_part(z_, y), wos.at[i], (wor if to_right else wol).at[k], right if to_right else left)

    def wo_y(z_, own=False):
        return remote(wo_mine() if own else wo_part(z_, y), wo_part(z_, y), woy_s.at[z_], woy_r.at[z_], ypeer)

    def wo_x(z_, y_):
        i = z_ + 4 * y_
        return remote(wo_part(z_, y_), wo_part(z_, y_), wox_s.at[i], wox_r.at[i], across)

    def wo_core(z_, y_, own=False):
        return remote(wo_ref if own else wo_whole(z_, y_), wo_whole(z_, y_), wod_s, wod_r, partner)

    def a_y(i):
        s, h = CHUNKS[i]
        return remote(a_st.at[s, 2 * (1 - y) + h], a_all.at[s, h, mine], ay_s.at[i], ay_r.at[i], ypeer)

    def a_line(i, k, to_right):
        s, h = CHUNKS[i]
        z_ = (z + 4 - k) % 4 if to_right else (z + k) % 4
        pair = a_all.at[s, h, pl.ds(place(z_, 0, c), 2)]
        return remote(pair, pair, as_.at[i * 6 + k + 3 * (not to_right)], (ar if to_right else al).at[i * 3 + k], right if to_right else left)

    def a_core(i, z_):
        s, h = CHUNKS[i]
        pair = a_all.at[s, h, pl.ds(place(z_, 0, c), 2)]
        return remote(pair, pair, ad_s.at[i], ad_r.at[i], partner)

    hu, hd = D // 2, FF // 2
    cu, cd = hu // UC, hd // UC

    def up_rows(n):
        return pl.ds(pl.multiple_of(group * hu + n * cu, 32), cu)

    def dn_rows(n):
        return pl.ds(pl.multiple_of(group * hd + n * cd, 16), cd)

    def yu(n):
        return remote(wup_ref.at[up_rows(n)], wu.at[1, up_rows(n)], yu_s.at[n], yu_r.at[n], ypeer)

    def xu(n):
        return remote(wu.at[1, up_rows(n)], wu.at[1, up_rows(n)], xu_s.at[n], xu_r.at[n], across)

    def yd(n):
        return remote(wdn_ref.at[dn_rows(n)], dn_out.at[dn_rows(n)], yd_s.at[n], yd_r.at[n], ypeer)

    def xd(n):
        return remote(dn_out.at[dn_rows(n)], dn_out.at[dn_rows(n)], xd_s.at[n], xd_r.at[n], across)

    def bias_flow():
        return remote(bup_ref, bu.at[1], b_s, b_r, ypeer)

    def hop(line, k, then):
        @pl.when(z >= k + 1)
        def _():
            line(k, True).wait_recv()

        if k < 2:
            go(lambda: line(k + 1, True), lambda: (z >= k + 1) & (z < 3))
        then((z + 3 - k) % 4, z >= k + 1)

        @pl.when(z <= 2 - k)
        def _():
            line(k, False).wait_recv()

        if k < 2:
            go(lambda: line(k + 1, False), lambda: (z <= 2 - k) & (z > 0))
        then((z + 1 + k) % 4, z <= 2 - k)

    def begin(line):
        go(lambda: line(0, True), lambda: z < 3)
        go(lambda: line(0, False), lambda: z > 0)

    def wo_then(z_, when):
        @pl.when(when)
        def _():
            wo_y(z_).start()
            wo_x(z_, y).start()

    def wo_hop(k):
        hop(wo_line, k, wo_then)

    def wo_from_y(k):
        def take(z_):
            wo_y(z_).wait_recv()
            wo_x(z_, 1 - y).start()

        if k == 0:
            take(z)
        else:
            @pl.when(z >= k)
            def _():
                take((z + 4 - k) % 4)

            @pl.when(z <= 3 - k)
            def _():
                take((z + k) % 4)

    def wo_from_x():
        for z_ in range(4):
            @pl.when(z_ != z)
            def _():
                wo_x(z_, y).wait_recv()
                wo_core(z_, y).start()
        for z_ in range(4):
            wo_x(z_, 1 - y).wait_recv()
            wo_core(z_, 1 - y).start()

    def a_send(i):
        go(functools.partial(a_y, i))

    def a_begin(i):
        a_y(i).wait_recv()
        begin(functools.partial(a_line, i))
        a_core(i, z).start()

    def a_hop(i, k):
        def then(z_, when):
            @pl.when(when)
            def _():
                a_core(i, z_).start()
        hop(functools.partial(a_line, i), k, then)

    barrier = pltpu.get_barrier_semaphore()
    peers = (partner, ypeer, across, right, left)
    for p in peers:
        pl.semaphore_signal(barrier, inc=1, device_id=p, device_id_type=MESH)

    def x_copy(g):
        return pltpu.make_async_copy(x_ref.at[g // PER_SEQ, pl.ds(pl.multiple_of((g % PER_SEQ) * TB, TB), TB)], xb.at[g % 2], xsem.at[g % 2])

    x_copy(0).start()
    locals_ = [pltpu.make_async_copy(wo_ref, wo_whole(z, y), wsem.at[0]), pltpu.make_async_copy(bup_ref, bu.at[0], wsem.at[1]), pltpu.make_async_copy(wup_ref, wu.at[0], wsem.at[2])]
    for copy in locals_:
        copy.start()
    row = lax.broadcasted_iota(jnp.int32, (KA - HD, S), 0)
    for h in range(2):
        q_s[h, HD:] = jnp.where(row == 0, 1.0, 0.0).astype(BF)
    pl.semaphore_wait(barrier, len(peers))

    begin(wo_line)
    wo_y(z, True).start()
    wo_core(z, y, True).start()
    go(bias_flow)

    x_copy(0).wait()
    x_copy(1).start()
    hid[0] = ln_rows(xb[0].astype(jnp.float32), ln1_gain, ln1_bias)

    def caches(s):
        return [pltpu.make_async_copy(k_s.at[:, pl.ds(0, HD)], k_out.at[s], csem.at[0]), pltpu.make_async_copy(v_s, v_out.at[s], csem.at[1])]

    def serve(table, *key):
        for at, todo in table.items():
            hit = functools.reduce(jnp.logical_and, [i == n for i, n in zip(key, at)])

            @pl.when(hit)
            def _():
                todo()

    def run(*todo):
        def all_of():
            for f, *args in todo:
                f(*args)
        return all_of

    def send(flow, n):
        go(functools.partial(flow, n))

    def pass_on(flow, onward, n):
        flow(n).wait_recv()
        go(functools.partial(onward, n))

    def await_all(flow):
        for n in range(UC):
            flow(n).wait_recv()

    IN_QKV = {
        (0, 6): run((wo_hop, 0), (wo_from_y, 0)),
        (1, 1): run((wo_from_y, 1)),
        (1, 4): run((wo_hop, 2), (send, yu, 0)),
        (1, 7): run((a_begin, 0), (a_begin, 1)),
        (2, 2): run((a_hop, 1, 0)),
        (2, 3): run((wo_from_y, 3)),
        (2, 4): run((a_hop, 0, 1)),
        (2, 5): run((send, yu, 2)),
        (2, 7): run((pass_on, yu, xu, 0)),
    }
    IN_ATTN = {
        (0, 3): run((a_send, 0), (a_send, 1), (wo_hop, 1)),
        (1, 1): run((wo_from_y, 2)),
        (1, 3): run((a_send, 2), (a_send, 3), (send, yu, 1), (a_hop, 0, 0)),
        (2, 0): run((a_hop, 1, 1)),
        (2, 1): run((a_begin, 2), (a_begin, 3)),
        (2, 2): run((a_hop, 0, 2), (pass_on, yu, xu, 1)),
        (2, 3): run((a_send, 4), (a_send, 5), (send, yu, 3)),
    }

    @pl.loop(0, NS)
    def _(s):
        n = lens_ref[s]

        @pl.when(s > 0)
        def _():
            for copy in caches(s - 1):
                copy.wait()

        @pl.loop(0, PER_SEQ)
        def _(b):
            g = s * PER_SEQ + b

            @pl.when(g + 1 < NS * PER_SEQ)
            def _():
                x_copy(g + 1).wait()

            @pl.when(g + 2 < NS * PER_SEQ)
            def _():
                x_copy(g + 2).start()

            cols = pl.ds(pl.multiple_of(b * TB, TB), TB)
            keep = b * TB + lax.broadcasted_iota(jnp.int32, (1, TB), 1) < n
            t = lax.dot_general(wq_ref[...], hid[g % 2], NT, preferred_element_type=jnp.float32)
            hid[(g + 1) % 2] = ln_rows(xb[(g + 1) % 2].astype(jnp.float32), ln1_gain, ln1_bias)
            t = (t + bq_ref[...]).astype(BF)
            for i in range(2):
                q_s[i, :HD, cols] = t[i * HD:(i + 1) * HD]
                k_s[i, :HD, cols] = jnp.where(keep, t[(2 + i) * HD:(3 + i) * HD], 0)
                v_s[i, :, cols] = jnp.where(keep, t[(4 + i) * HD:(5 + i) * HD], 0)
            serve(IN_QKV, s, b)

        pos = lax.broadcasted_iota(jnp.int32, (KA - HD, S), 1)
        for i in range(2):
            k_s[i, HD:] = jnp.where((row == 0) & (pos >= n), -1e30, 0.0).astype(BF)
            kt[i] = k_s[i].T
        for copy in caches(s):
            copy.start()

        causal = lax.broadcasted_iota(jnp.int32, (QB, QB), 0) <= lax.broadcasted_iota(jnp.int32, (QB, QB), 1)

        @pl.loop(0, 4)
        def _(t):
            at_q = pl.ds(pl.multiple_of(t * QB, QB), QB)

            def block(h, j, m, l, acc, masked):
                at = pl.ds(pl.multiple_of(j * QB, QB), QB)
                sc = jnp.dot(kt[h, at], q_s[h, :, at_q], preferred_element_type=jnp.float32) * (SCALE * LOG2E)
                if masked:
                    sc = jnp.where(causal, sc, -1e30)
                m_new = jnp.maximum(m, jnp.max(sc, axis=0, keepdims=True))
                p = jnp.exp2(sc - m_new)
                scale = jnp.exp2(m - m_new)
                l = scale * l + jnp.sum(p, axis=0, keepdims=True)
                acc = scale * acc + jnp.dot(v_s[h, :, at], p.astype(BF), preferred_element_type=jnp.float32)
                return m_new, l, acc

            zero = (jnp.full((1, QB), -1e30, jnp.float32), jnp.zeros((1, QB), jnp.float32), jnp.zeros((HD, QB), jnp.float32))
            carry = lax.fori_loop(0, t, lambda j, c: tuple(block(h, j, *c[h], False) for h in range(2)), (zero, zero))
            for h in range(2):
                _, l, acc = block(h, t, *carry[h], True)
                a_st[s, t, h * HD:(h + 1) * HD] = (acc / l).astype(BF)

            @pl.when(t // 2 == y)
            def _():
                a_all[s, t % 2, mine] = a_st[s, t]

            serve(IN_ATTN, s, t)

    per = QB // TB
    n_blocks = NS * 2 * per

    def res_copy(i):
        rows = pl.ds(pl.multiple_of(y * (S // 2) + (i % (2 * per)) * TB, TB), TB)
        return pltpu.make_async_copy(x_ref.at[i // (2 * per), rows], xb.at[i % 2], xsem.at[i % 2])

    def put_x1(i):
        return pltpu.make_async_copy(st1.at[i % 2], x1_out.at[pl.ds(pl.multiple_of(i * TB, TB), TB)], osem.at[i % 2])

    def put_u(i):
        return pltpu.make_async_copy(st2.at[i % 2], u_out.at[pl.ds(pl.multiple_of(i * TB, TB), TB)], lsem.at[i % 2])

    def a_ready(i):
        s, h = CHUNKS[i]
        whole = a_all.at[s, h, pl.ds(0, 8)]
        pltpu.make_async_copy(whole, whole, ad_r.at[i]).wait()

    whole = wt.at[pl.ds(0, D // 2)]

    def wo_ready():
        pltpu.make_async_copy(whole, whole, wod_r).wait()
        bias_flow().wait_recv()
        for copy in locals_:
            copy.wait()

    res_copy(0).start()
    run((wo_from_x,), (a_hop, 1, 2), (pass_on, yu, xu, 2), (a_hop, 2, 0), (wo_ready,))()
    for n in range(UC):
        send(yd, n)

    BEFORE = {
        (0,): run((a_ready, 0)),
        (1,): run((a_hop, 3, 0), (pass_on, yu, xu, 3)),
        (2,): run((a_ready, 1), (a_hop, 2, 1)),
        (3,): run((a_hop, 3, 1), (a_begin, 4), (a_begin, 5)),
        (4,): run((await_all, xu), (a_hop, 2, 2), (a_ready, 2)),
        (5,): run((a_hop, 3, 2)),
        (6,): run((a_ready, 3), (a_hop, 4, 0), (a_hop, 5, 0)),
        (7,): run((a_hop, 4, 1), (a_hop, 5, 1), *((pass_on, yd, xd, n) for n in range(UC))),
        (8,): run((a_hop, 4, 2), (a_ready, 4)),
        (9,): run((a_hop, 5, 2)),
        (10,): run((a_ready, 5)),
    }

    def up_proj(b):
        @pl.when(b >= 2)
        def _():
            put_u(b - 2).wait()

        for n in range(2):
            up = jnp.dot(hid[b % RING], wu[n], preferred_element_type=jnp.float32) + bu[n, 0:1]
            st2[b % 2, :, n * FF:(n + 1) * FF] = jnp.maximum(up, 0).astype(BF)
        put_u(b).start()

    def out_proj(b):
        a = a_all[b // (2 * per), (b // per) % 2, :, :, pl.ds(pl.multiple_of((b % per) * TB, TB), TB)].reshape(D, TB)
        return lax.dot_general(a, wt[...], TN, preferred_element_type=jnp.float32)

    def residual(b, o):
        x1 = (xb[b % 2].astype(jnp.float32) + o + b_out).astype(BF)
        st1[b % 2] = x1
        hid[b % RING] = ln_rows(x1.astype(jnp.float32), ln2_gain, ln2_bias)

    def next_rows(b):
        res_copy(b).wait()

        @pl.when(b + 1 < n_blocks)
        def _():
            res_copy(b + 1).start()

    @pl.loop(0, n_blocks)
    def _(b):
        serve(BEFORE, b)
        next_rows(b)

        @pl.when(b >= 2)
        def _():
            put_x1(b - 2).wait()

        residual(b, out_proj(b))
        put_x1(b).start()

        @pl.when((b >= LAG) & (b < 2 * LAG - 1))
        def _():
            up_proj(2 * (b - LAG))
            up_proj(2 * (b - LAG) + 1)

        @pl.when(b >= 2 * LAG - 1)
        def _():
            up_proj(b - 1)

    up_proj(n_blocks - 1)
    await_all(xd)
    for b in range(n_blocks - 2, n_blocks):
        put_x1(b).wait()
        put_u(b).wait()
    for copy in caches(NS - 1):
        copy.wait()
    for make, when in sent:
        if when is None:
            make().wait_send()
        else:
            @pl.when(when())
            def _():
                make().wait_send()
    for z_ in range(4):
        wo_y(z_).wait_send()
        wo_x(z_, 1 - y).wait_send()

        @pl.when(z_ != z)
        def _():
            wo_x(z_, y).wait_send()
    pltpu.make_async_copy(whole, whole, wod_s).wait()
    for i, (s, h) in enumerate(CHUNKS):
        pairs = a_all.at[s, h, pl.ds(0, 8)]
        pltpu.make_async_copy(pairs, pairs, ad_s.at[i]).wait()


def front(lens, x, vec, wq, bq, wo, wup, bup, wdn):
    v = pl.BlockSpec(memory_space=pltpu.VMEM)
    sem = lambda n: pltpu.SemaphoreType.DMA((n,))
    one = pltpu.SemaphoreType.DMA
    cache = jax.ShapeDtypeStruct((NS, 2, HD, S), BF)
    rows = lambda n: jax.ShapeDtypeStruct((NS * S // 2, n), BF)
    nc = len(CHUNKS)
    return pl.pallas_call(
        front_kernel,
        out_shape=(cache, cache, rows(D), rows(2 * FF), jax.ShapeDtypeStruct((FF, D), BF)),
        in_specs=[pl.BlockSpec(memory_space=pltpu.SMEM), ANY, v, v, v, ANY, ANY, ANY, ANY],
        out_specs=(ANY,) * 5,
        scratch_shapes=[
            pltpu.VMEM((D, D), BF), pltpu.VMEM((2, D, FF), BF), pltpu.VMEM((NS, 2, 16, 2 * HD, QB), BF), pltpu.VMEM((2, TB, D), BF),
            pltpu.VMEM((2, KA, S), BF), pltpu.VMEM((2, KA, S), BF), pltpu.VMEM((2, HD, S), BF), pltpu.VMEM((2, S, KA), BF),
            pltpu.VMEM((NS, 4, 2 * HD, QB), BF), pltpu.VMEM((2, 8, FF), jnp.float32), pltpu.VMEM((2, TB, D), BF), pltpu.VMEM((2, TB, 2 * FF), BF), pltpu.VMEM((RING, TB, D), BF),
            sem(2), sem(2), sem(2), sem(2), sem(3), sem(6), sem(3), sem(3), sem(4), sem(4), sem(8), sem(8), one, one, sem(nc), sem(nc), sem(6 * nc), sem(3 * nc), sem(3 * nc), sem(nc), sem(nc),
            one, one, sem(UC), sem(UC), sem(UC), sem(UC), sem(UC), sem(UC), sem(UC), sem(UC),
        ],
        compiler_params=pltpu.CompilerParams(collective_id=1, has_side_effects=True, vmem_limit_bytes=63 * 2**20),
        cost_estimate=pl.CostEstimate(flops=10**11, bytes_accessed=10**8, transcendentals=0),
        name="front",
    )(lens, x, vec, wq, bq, wo, wup, bup, wdn)


BR = 128
NB = 3 * S // 2 // BR
Q = BR // 8
CH = BR // 2
SLOTS, S1N = 6, 4


def down_kernel(u_ref, w0_ref, w1_ref, x1_ref, bd_ref, o_ref,
                wd, ub, x1b, pt, acc, s1, r1, sm, rr, rl, fin,
                wsem, usem, xsem, lsem, s1s, r1s, sms, rrs, rls, zs, frs, fls, ys, yr, ds, dr):
    group, me = lax.axis_index("dp"), lax.axis_index("tp")
    z, y, c = me // 4, (me // 2) % 2, me % 2
    dev = lambda z_, y_, c_: (group, z_ * 4 + y_ * 2 + c_)
    partner, ypeer = dev(z, y, 1 - c), dev(z, 1 - y, c)
    right, left = dev((z + 1) % 4, y, c), dev((z + 3) % 4, y, c)

    barrier = pltpu.get_barrier_semaphore()
    for peer in (partner, ypeer, right, left):
        pl.semaphore_signal(barrier, inc=1, device_id=peer, device_id_type=MESH)

    loads = [pltpu.make_async_copy(w, wd.at[pl.ds(i * FF, FF)], wsem.at[i]) for i, w in enumerate((w0_ref, w1_ref))]
    for copy in loads:
        copy.start()

    def u_load(b):
        return pltpu.make_async_copy(u_ref.at[pl.ds(pl.multiple_of(b * BR, BR), BR)], ub.at[b], usem.at[b])

    def x1_load(b):
        rows = pl.ds(pl.multiple_of(b * BR + c * CH + z * Q, Q), Q)
        return pltpu.make_async_copy(x1_ref.at[rows], x1b.at[b], xsem.at[b])

    @pl.loop(0, NB)
    def _(b):
        u_load(b).start()
        x1_load(b).start()

    for copy in loads:
        copy.wait()
    pl.semaphore_wait(barrier, 4)

    per = NB // 3

    def rows_of(b, z_, y_):
        pos = (S // 2) * y_ + BR * (b % per) + CH * c + Q * z_
        return pl.ds(pl.multiple_of((b // per) * S + pos, Q), Q)

    def remote(src, dst, ss, rs, to):
        return pltpu.make_async_remote_copy(src, dst, ss, rs, device_id=to, device_id_type=MESH)

    def swap(b):
        return remote(s1.at[b % S1N], r1.at[b], s1s.at[b % S1N], r1s.at[b], partner)

    def chain(b, n, at, to_right):
        dst, sem = (rr, rrs) if to_right else (rl, rls)
        return remote(sm.at[b, pl.ds(at, n * Q)], dst.at[b, pl.ds(0, n * Q)], sms, sem.at[b], right if to_right else left)

    def go_right(b, k):
        rows = rows_of(b, (z + 4 - k) % 4, y)
        return remote(fin.at[b] if k == 0 else o_ref.at[rows], o_ref.at[rows], zs, frs.at[b * 3 + k], right)

    def go_left(b, k):
        rows = rows_of(b, (z + k) % 4, y)
        return remote(fin.at[b] if k == 0 else o_ref.at[rows], o_ref.at[rows], zs, fls.at[b * 3 + k], left)

    def go_y(b, z_, own=False):
        rows = rows_of(b, z_, y)
        return remote(fin.at[b] if own else o_ref.at[rows], o_ref.at[rows], ys, yr.at[b * 4 + z_], ypeer)

    def go_core(b, z_, y_, own=False):
        rows = rows_of(b, z_, y_)
        return remote(fin.at[b] if own else o_ref.at[rows], o_ref.at[rows], ds, dr, partner)

    f32 = lambda v: v.astype(jnp.float32)

    def multiply(b):
        u_load(b).wait()

        @pl.when(b >= S1N)
        def _():
            swap(b - S1N).wait_send()

        @pl.loop(0, 5)
        def _(j):
            cols = pl.ds(pl.multiple_of(j * 512, 512), 512)
            pt[...] = jnp.dot(ub[b], wd[:, cols], preferred_element_type=jnp.float32)
            acc[b % SLOTS, :, cols] = pt[pl.ds(pl.multiple_of(c * CH, CH), CH)]
            s1[b % S1N, :, cols] = pt[pl.ds(pl.multiple_of((1 - c) * CH, CH), CH)].astype(BF)

        swap(b).start()

    def own(i, n=1):
        return slice(i * Q, (i + n) * Q)

    def stage2(b):
        swap(b).wait_recv()
        acc[b % SLOTS] += f32(r1[b])

        @pl.when(z == 0)
        def _():
            sm[b] = acc[b % SLOTS, own(1, 3)].astype(BF)
            chain(b, 3, 0, True).start()

        @pl.when(z == 3)
        def _():
            sm[b] = acc[b % SLOTS, own(0, 3)].astype(BF)
            chain(b, 3, 0, False).start()

    def stage3(b):
        a = acc.at[b % SLOTS]

        @pl.when(z == 1)
        def _():
            chain(b, 3, 0, True).wait_recv()
            a[own(1)] += f32(rr[b, own(0)])
            sm[b, own(0, 2)] = (a[own(2, 2)] + f32(rr[b, own(1, 2)])).astype(BF)
            chain(b, 2, 0, True).start()

        @pl.when(z == 2)
        def _():
            chain(b, 3, 0, False).wait_recv()
            a[own(2)] += f32(rl[b, own(2)])
            sm[b, own(0, 2)] = (a[own(0, 2)] + f32(rl[b, own(0, 2)])).astype(BF)
            chain(b, 2, 0, False).start()

    def stage4(b):
        a = acc.at[b % SLOTS]

        @pl.when(z == 2)
        def _():
            chain(b, 2, 0, True).wait_recv()
            a[own(2)] += f32(rr[b, own(0)])
            sm[b, own(2)] = (a[own(3)] + f32(rr[b, own(1)])).astype(BF)
            chain(b, 1, 2 * Q, True).start()

        @pl.when(z == 1)
        def _():
            chain(b, 2, 0, False).wait_recv()
            a[own(1)] += f32(rl[b, own(1)])
            sm[b, own(2)] = (a[own(0)] + f32(rl[b, own(0)])).astype(BF)
            chain(b, 1, 2 * Q, False).start()

    def finish(b):
        a = acc.at[b % SLOTS]

        @pl.when(z == 3)
        def _():
            chain(b, 1, 2 * Q, True).wait_recv()
            a[own(3)] += f32(rr[b, own(0)])

        @pl.when(z == 0)
        def _():
            chain(b, 1, 2 * Q, False).wait_recv()
            a[own(0)] += f32(rl[b, own(0)])

        x1_load(b).wait()
        down = a[pl.ds(pl.multiple_of(z * Q, Q), Q)] + bd_ref[...]
        fin[b] = (f32(x1b[b]) + down).astype(BF)
        go_y(b, z, True).start()

        @pl.when(z < 3)
        def _():
            go_right(b, 0).start()

        @pl.when(z > 0)
        def _():
            go_left(b, 0).start()

        go_core(b, z, y, True).start()
        pltpu.make_async_copy(fin.at[b], o_ref.at[rows_of(b, z, y)], lsem).start()

    def relay(b, k):
        @pl.when(z >= k + 1)
        def _():
            go_right(b, k).wait_recv()
            if k < 2:
                @pl.when(z < 3)
                def _():
                    go_right(b, k + 1).start()
            go_y(b, (z + 3 - k) % 4).start()
            go_core(b, (z + 3 - k) % 4, y).start()

        @pl.when(z <= 2 - k)
        def _():
            go_left(b, k).wait_recv()
            if k < 2:
                @pl.when(z > 0)
                def _():
                    go_left(b, k + 1).start()
            go_y(b, (z + 1 + k) % 4).start()
            go_core(b, (z + 1 + k) % 4, y).start()

    def across(b):
        for z_ in range(4):
            go_y(b, z_).wait_recv()
            go_core(b, z_, 1 - y).start()

    stages = (multiply, stage2, stage3, stage4, finish, functools.partial(relay, k=0), functools.partial(relay, k=1), functools.partial(relay, k=2), across)

    @pl.loop(0, NB + len(stages) - 1)
    def _(t):
        for i, stage in enumerate(stages):
            b = t - i

            @pl.when((b >= 0) & (b < NB))
            def _():
                stage(b)

    def drain(sem, n):
        rows = o_ref.at[pl.ds(0, n)]
        pltpu.make_async_copy(rows, rows, sem).wait()

    n = NB * Q
    drain(dr, 8 * n)
    drain(ds, 8 * n)
    drain(ys, 4 * n)
    drain(lsem, n)
    drain(sms, 3 * n)
    ends = (z == 0) | (z == 3)

    @pl.when(ends)
    def _():
        drain(zs, n)

    @pl.when(jnp.logical_not(ends))
    def _():
        drain(zs, 5 * n)

    for b in range(NB - S1N, NB):
        swap(b).wait_send()


def down(u, w0, w1, x1, bd):
    sem = lambda n: pltpu.SemaphoreType.DMA((n,))
    one = pltpu.SemaphoreType.DMA
    return pl.pallas_call(
        down_kernel,
        out_shape=jax.ShapeDtypeStruct((3 * S, D), BF),
        in_specs=[ANY] * 4 + [pl.BlockSpec(memory_space=pltpu.VMEM)],
        out_specs=ANY,
        scratch_shapes=[
            pltpu.VMEM((2 * FF, D), BF), pltpu.VMEM((NB, BR, 2 * FF), BF), pltpu.VMEM((NB, Q, D), BF), pltpu.VMEM((BR, 512), jnp.float32),
            pltpu.VMEM((SLOTS, CH, D), jnp.float32), pltpu.VMEM((S1N, CH, D), BF), pltpu.VMEM((NB, CH, D), BF),
            pltpu.VMEM((NB, 3 * Q, D), BF), pltpu.VMEM((NB, 3 * Q, D), BF), pltpu.VMEM((NB, 3 * Q, D), BF), pltpu.VMEM((NB, Q, D), BF),
            sem(2), sem(NB), sem(NB), one, sem(S1N), sem(NB), one, sem(NB), sem(NB), one, sem(3 * NB), sem(3 * NB), one, sem(4 * NB), one, one,
        ],
        compiler_params=pltpu.CompilerParams(collective_id=0, has_side_effects=True, vmem_limit_bytes=62 * 2**20),
        cost_estimate=pl.CostEstimate(flops=4 * S * D * D, bytes_accessed=4 * D * D, transcendentals=0),
        name="down",
    )(u, w0, w1, x1, bd)


def solution(mesh):
    def local_layer(x_in, seq_lens, ln1_gain, ln1_bias, w_qkv, b_qkv, w_out, b_out, ln2_gain, ln2_bias, w_up, b_up, w_down, b_down):
        f32 = lambda v: v.astype(jnp.float32)
        wq = jnp.transpose(w_qkv, (1, 2, 3, 0)).reshape(6 * HD, D)
        bq = f32(b_qkv).reshape(6 * HD, 1)
        vec = jnp.stack([ln1_gain, ln1_bias, f32(b_out), ln2_gain, ln2_bias, f32(b_down)])
        bup = jnp.broadcast_to(f32(b_up)[None], (8, FF))
        keys, values, x1, u, down_y = front(seq_lens, x_in, vec, wq, bq, w_out.reshape(2 * HD, D), w_up, bup, w_down)
        x_out = down(u, w_down, down_y, x1, vec[5:6]).reshape(x_in.shape)
        return x_out, jnp.swapaxes(keys, 2, 3), jnp.swapaxes(values, 2, 3)

    arg_specs = (P("dp", None, None), P("dp"), P(), P(), P(None, None, "tp", None), P(None, "tp", None), P("tp", None, None), P(), P(), P(), P(None, "tp"), P("tp"), P("tp", None), P())
    cache_spec = P("dp", "tp", None, None)
    return jax.shard_map(local_layer, mesh=mesh, in_specs=arg_specs, out_specs=(P("dp", None, None), cache_spec, cache_spec), check_vma=False)
```

```python
import functools

import jax
import jax.numpy as jnp
from jax import lax
from jax.experimental import pallas as pl
from jax.experimental.pallas import tpu as pltpu
from jax.sharding import PartitionSpec as P

D, S, HD, FF = 2560, 2048, 80, 640
BF = jnp.bfloat16
MESH = pl.DeviceIdType.MESH
ANY = pl.BlockSpec(memory_space=pl.ANY)
NT = (((1,), (1,)), ((), ()))
TN = (((0,), (0,)), ((), ()))
SCALE = HD ** -0.5
LOG2E = 1.4426950408889634


def ln_rows(x, gain, bias):
    centered = x - jnp.mean(x, axis=-1, keepdims=True)
    var = jnp.mean(centered * centered, axis=-1, keepdims=True)
    return (centered * lax.rsqrt(var + 1e-5) * gain + bias).astype(BF)


TB, KA, NS = 256, 96, 3
QB = S // 4
PER_SEQ = S // TB
UC = 4
LAG = 4
RING = LAG + 1
DOWN, UP, QKV = 5, 6, 7
IN_QKV = {"0.6": "w0 v0", "1.1": "v1", "1.4": "w2 u0", "1.7": "b0 b1", "2.2": "h10", "2.3": "v3", "2.4": "h01", "2.5": "u2", "2.7": "p0"}
IN_ATTN = {"0.3": "s0 s1 w1", "1.1": "v2", "1.3": "s2 s3 u1 h00", "2.0": "h11", "2.1": "b2 b3", "2.2": "h02 p1", "2.3": "s4 s5 u3"}
AFTER = "x h12 p2 h20 o"
BEFORE = {"0": "r0", "1": "h30 p3", "2": "r1 h21", "3": "h31 b4", "4": "q h22 r2", "5": "h32 h40 b5", "6": "r3 h41", "7": "h50 h42 d", "8": "r4 h51", "9": "h52", "10": "r5"}
CHUNKS = tuple((s, h) for s in range(NS) for h in range(2))


def front_kernel(lens_ref, x_ref, vec_ref, wq_ref, wo_ref, wup_ref, wdn_ref,
                 k_out, v_out, x1_out, u_out, dn_out,
                 wt, wu, a_all, xb, q_s, k_s, v_s, kt, a_st, bu, st1, st2, hid,
                 xsem, csem, osem, lsem, wsem, wos, wor, wol, woy_s, woy_r, wox_s, wox_r, wod_s, wod_r, ay_s, ay_r, as_, ar, al, ad_s, ad_r,
                 b_s, b_r, yu_s, yu_r, yd_s, yd_r, xu_s, xu_r, xd_s, xd_r):
    group, me = lax.axis_index("dp"), lax.axis_index("tp")
    z, y, c = me // 4, (me // 2) % 2, me % 2
    dev = lambda z_, y_, c_: (group, z_ * 4 + y_ * 2 + c_)
    partner, ypeer, across = dev(z, y, 1 - c), dev(z, 1 - y, c), (1 - group, me)
    right, left = dev((z + 1) % 4, y, c), dev((z + 3) % 4, y, c)
    ln1_gain, ln1_bias, b_out, ln2_gain, ln2_bias = (vec_ref[i:i + 1] for i in range(5))
    b_qkv = vec_ref[:, :512].T[:6 * HD, QKV:QKV + 1]
    sent = []

    def remote(src, dst, ss, rs, to):
        return pltpu.make_async_remote_copy(src, dst, ss, rs, device_id=to, device_id_type=MESH)

    def go(make, when=None):
        if when is None:
            make().start()
        else:
            @pl.when(when())
            def _():
                make().start()
        sent.append((make, when))

    place = lambda z_, y_, c_: (z_ * 2 + c_) * 2 + y_
    mine = place(z, y, c)
    half = HD

    def wo_part(z_, y_):
        return wt.at[pl.ds(pl.multiple_of(place(z_, y_, c) * 2 * HD + group * half, 16), half)]

    def wo_whole(z_, y_):
        return wt.at[pl.ds(pl.multiple_of(place(z_, y_, c) * 2 * HD, 32), 2 * HD)]

    def wo_mine():
        return wo_ref.at[pl.ds(pl.multiple_of(group * half, 16), half)]

    def wo_line(k, to_right):
        z_ = (z + 4 - k) % 4 if to_right else (z + k) % 4
        i = k + 3 * (not to_right)
        return remote(wo_mine() if k == 0 else wo_part(z_, y), wo_part(z_, y), wos.at[i], (wor if to_right else wol).at[k], right if to_right else left)

    def wo_y(z_, own=False):
        return remote(wo_mine() if own else wo_part(z_, y), wo_part(z_, y), woy_s.at[z_], woy_r.at[z_], ypeer)

    def wo_x(z_, y_):
        i = z_ + 4 * y_
        return remote(wo_part(z_, y_), wo_part(z_, y_), wox_s.at[i], wox_r.at[i], across)

    def wo_core(z_, y_, own=False):
        return remote(wo_ref if own else wo_whole(z_, y_), wo_whole(z_, y_), wod_s, wod_r, partner)

    def a_y(i):
        s, h = CHUNKS[i]
        return remote(a_st.at[s, 2 * (1 - y) + h], a_all.at[s, h, mine], ay_s.at[i], ay_r.at[i], ypeer)

    def a_line(i, k, to_right):
        s, h = CHUNKS[i]
        z_ = (z + 4 - k) % 4 if to_right else (z + k) % 4
        pair = a_all.at[s, h, pl.ds(place(z_, 0, c), 2)]
        return remote(pair, pair, as_.at[i * 6 + k + 3 * (not to_right)], (ar if to_right else al).at[i * 3 + k], right if to_right else left)

    def a_core(i, z_):
        s, h = CHUNKS[i]
        pair = a_all.at[s, h, pl.ds(place(z_, 0, c), 2)]
        return remote(pair, pair, ad_s.at[i], ad_r.at[i], partner)

    hu, hd = D // 2, FF // 2
    cu, cd = hu // UC, hd // UC

    def up_rows(n):
        return pl.ds(pl.multiple_of(group * hu + n * cu, 32), cu)

    def dn_rows(n):
        return pl.ds(pl.multiple_of(group * hd + n * cd, 16), cd)

    def yu(n):
        return remote(wup_ref.at[up_rows(n)], wu.at[1, up_rows(n)], yu_s.at[n], yu_r.at[n], ypeer)

    def xu(n):
        return remote(wu.at[1, up_rows(n)], wu.at[1, up_rows(n)], xu_s.at[n], xu_r.at[n], across)

    def yd(n):
        return remote(wdn_ref.at[dn_rows(n)], dn_out.at[dn_rows(n)], yd_s.at[n], yd_r.at[n], ypeer)

    def xd(n):
        return remote(dn_out.at[dn_rows(n)], dn_out.at[dn_rows(n)], xd_s.at[n], xd_r.at[n], across)

    def bias_flow():
        return remote(vec_ref.at[:, pl.ds(0, FF)], bu, b_s, b_r, ypeer)

    def hop(line, k, then):
        @pl.when(z >= k + 1)
        def _():
            line(k, True).wait_recv()

        if k < 2:
            go(lambda: line(k + 1, True), lambda: (z >= k + 1) & (z < 3))
        then((z + 3 - k) % 4, z >= k + 1)

        @pl.when(z <= 2 - k)
        def _():
            line(k, False).wait_recv()

        if k < 2:
            go(lambda: line(k + 1, False), lambda: (z <= 2 - k) & (z > 0))
        then((z + 1 + k) % 4, z <= 2 - k)

    def begin(line):
        go(lambda: line(0, True), lambda: z < 3)
        go(lambda: line(0, False), lambda: z > 0)

    def wo_then(z_, when):
        @pl.when(when)
        def _():
            wo_y(z_).start()
            wo_x(z_, y).start()

    def wo_hop(k):
        hop(wo_line, k, wo_then)

    def wo_from_y(k):
        def take(z_):
            wo_y(z_).wait_recv()
            wo_x(z_, 1 - y).start()

        if k == 0:
            take(z)
        else:
            @pl.when(z >= k)
            def _():
                take((z + 4 - k) % 4)

            @pl.when(z <= 3 - k)
            def _():
                take((z + k) % 4)

    def wo_from_x():
        for z_ in range(4):
            @pl.when(z_ != z)
            def _():
                wo_x(z_, y).wait_recv()
                wo_core(z_, y).start()
        for z_ in range(4):
            wo_x(z_, 1 - y).wait_recv()
            wo_core(z_, 1 - y).start()

    def a_send(i):
        go(functools.partial(a_y, i))

    def a_begin(i):
        a_y(i).wait_recv()
        begin(functools.partial(a_line, i))
        a_core(i, z).start()

    def a_hop(i, k):
        def then(z_, when):
            @pl.when(when)
            def _():
                a_core(i, z_).start()
        hop(functools.partial(a_line, i), k, then)

    barrier = pltpu.get_barrier_semaphore()
    peers = (partner, ypeer, across, right, left)
    for p in peers:
        pl.semaphore_signal(barrier, inc=1, device_id=p, device_id_type=MESH)

    def x_copy(g):
        return pltpu.make_async_copy(x_ref.at[g // PER_SEQ, pl.ds(pl.multiple_of((g % PER_SEQ) * TB, TB), TB)], xb.at[g % 2], xsem.at[g % 2])

    x_copy(0).start()
    locals_ = [pltpu.make_async_copy(wo_ref, wo_whole(z, y), wsem.at[0]), pltpu.make_async_copy(wup_ref, wu.at[0], wsem.at[1])]
    for copy in locals_:
        copy.start()
    row = lax.broadcasted_iota(jnp.int32, (KA - HD, S), 0)
    for h in range(2):
        q_s[h, HD:] = jnp.where(row == 0, 1.0, 0.0).astype(BF)
    pl.semaphore_wait(barrier, len(peers))

    begin(wo_line)
    wo_y(z, True).start()
    wo_core(z, y, True).start()
    go(bias_flow)

    x_copy(0).wait()
    x_copy(1).start()
    hid[0] = ln_rows(xb[0].astype(jnp.float32), ln1_gain, ln1_bias)

    def caches(s):
        return [pltpu.make_async_copy(k_s.at[:, pl.ds(0, HD)], k_out.at[s], csem.at[0]), pltpu.make_async_copy(v_s, v_out.at[s], csem.at[1])]

    def send(flow, n):
        go(functools.partial(flow, n))

    def pass_on(flow, onward, n):
        flow(n).wait_recv()
        go(functools.partial(onward, n))

    def await_all(flow):
        for n in range(UC):
            flow(n).wait_recv()

    whole = wt.at[pl.ds(0, D // 2)]

    def wo_ready():
        pltpu.make_async_copy(whole, whole, wod_r).wait()
        bias_flow().wait_recv()
        for copy in locals_:
            copy.wait()

    def a_ready(i):
        s, h = CHUNKS[i]
        pairs = a_all.at[s, h, pl.ds(0, 8)]
        pltpu.make_async_copy(pairs, pairs, ad_r.at[i]).wait()

    def down_over():
        for n in range(UC):
            pass_on(yd, xd, n)

    todo = {
        "w": wo_hop, "v": wo_from_y, "x": wo_from_x, "o": wo_ready,
        "s": a_send, "b": a_begin, "h": a_hop, "r": a_ready,
        "u": functools.partial(send, yu), "p": functools.partial(pass_on, yu, xu), "q": functools.partial(await_all, xu),
        "d": down_over,
    }

    def run(words):
        for w in words.split():
            todo[w[0]](*map(int, w[1:]))

    def serve(table, *key):
        for at, words in table.items():
            @pl.when(functools.reduce(jnp.logical_and, [i == int(n) for i, n in zip(key, at.split("."))]))
            def _():
                run(words)

    @pl.loop(0, NS)
    def _(s):
        n = lens_ref[s]

        @pl.when(s > 0)
        def _():
            for copy in caches(s - 1):
                copy.wait()

        @pl.loop(0, PER_SEQ)
        def _(b):
            g = s * PER_SEQ + b

            @pl.when(g + 1 < NS * PER_SEQ)
            def _():
                x_copy(g + 1).wait()

            @pl.when(g + 2 < NS * PER_SEQ)
            def _():
                x_copy(g + 2).start()

            cols = pl.ds(pl.multiple_of(b * TB, TB), TB)
            keep = b * TB + lax.broadcasted_iota(jnp.int32, (1, TB), 1) < n
            t = lax.dot_general(wq_ref[...], hid[g % 2], NT, preferred_element_type=jnp.float32)
            hid[(g + 1) % 2] = ln_rows(xb[(g + 1) % 2].astype(jnp.float32), ln1_gain, ln1_bias)
            t = (t + b_qkv).astype(BF)
            for i in range(2):
                q_s[i, :HD, cols] = t[i * HD:(i + 1) * HD]
                k_s[i, :HD, cols] = jnp.where(keep, t[(2 + i) * HD:(3 + i) * HD], 0)
                v_s[i, :, cols] = jnp.where(keep, t[(4 + i) * HD:(5 + i) * HD], 0)
            serve(IN_QKV, s, b)

        pos = lax.broadcasted_iota(jnp.int32, (KA - HD, S), 1)
        for i in range(2):
            k_s[i, HD:] = jnp.where((row == 0) & (pos >= n), -1e30, 0.0).astype(BF)
            kt[i] = k_s[i].T
        for copy in caches(s):
            copy.start()

        causal = lax.broadcasted_iota(jnp.int32, (QB, QB), 0) <= lax.broadcasted_iota(jnp.int32, (QB, QB), 1)

        @pl.loop(0, 4)
        def _(t):
            at_q = pl.ds(pl.multiple_of(t * QB, QB), QB)

            def block(h, j, m, l, acc, masked):
                at = pl.ds(pl.multiple_of(j * QB, QB), QB)
                sc = jnp.dot(kt[h, at], q_s[h, :, at_q], preferred_element_type=jnp.float32) * (SCALE * LOG2E)
                if masked:
                    sc = jnp.where(causal, sc, -1e30)
                m_new = jnp.maximum(m, jnp.max(sc, axis=0, keepdims=True))
                p = jnp.exp2(sc - m_new)
                scale = jnp.exp2(m - m_new)
                l = scale * l + jnp.sum(p, axis=0, keepdims=True)
                acc = scale * acc + jnp.dot(v_s[h, :, at], p.astype(BF), preferred_element_type=jnp.float32)
                return m_new, l, acc

            zero = (jnp.full((1, QB), -1e30, jnp.float32), jnp.zeros((1, QB), jnp.float32), jnp.zeros((HD, QB), jnp.float32))
            carry = lax.fori_loop(0, t, lambda j, c: tuple(block(h, j, *c[h], False) for h in range(2)), (zero, zero))
            for h in range(2):
                _, l, acc = block(h, t, *carry[h], True)
                a_st[s, t, h * HD:(h + 1) * HD] = (acc / l).astype(BF)

            @pl.when(t // 2 == y)
            def _():
                a_all[s, t % 2, mine] = a_st[s, t]

            serve(IN_ATTN, s, t)

    per = QB // TB
    n_blocks = NS * 2 * per

    def res_copy(i):
        rows = pl.ds(pl.multiple_of(y * (S // 2) + (i % (2 * per)) * TB, TB), TB)
        return pltpu.make_async_copy(x_ref.at[i // (2 * per), rows], xb.at[i % 2], xsem.at[i % 2])

    def put_x1(i):
        return pltpu.make_async_copy(st1.at[i % 2], x1_out.at[pl.ds(pl.multiple_of(i * TB, TB), TB)], osem.at[i % 2])

    def put_u(i):
        return pltpu.make_async_copy(st2.at[i % 2], u_out.at[pl.ds(pl.multiple_of(i * TB, TB), TB)], lsem.at[i % 2])

    res_copy(0).start()
    run(AFTER)
    for n in range(UC):
        send(yd, n)

    def up_proj(b):
        @pl.when(b >= 2)
        def _():
            put_u(b - 2).wait()

        for n in range(2):
            up = jnp.dot(hid[b % RING], wu[n], preferred_element_type=jnp.float32) + (bu if n else vec_ref)[UP:UP + 1, :FF]
            st2[b % 2, :, n * FF:(n + 1) * FF] = jnp.maximum(up, 0).astype(BF)
        put_u(b).start()

    def out_proj(b):
        a = a_all[b // (2 * per), (b // per) % 2, :, :, pl.ds(pl.multiple_of((b % per) * TB, TB), TB)].reshape(D, TB)
        return lax.dot_general(a, wt[...], TN, preferred_element_type=jnp.float32)

    def residual(b, o):
        x1 = (xb[b % 2].astype(jnp.float32) + o + b_out).astype(BF)
        st1[b % 2] = x1
        hid[b % RING] = ln_rows(x1.astype(jnp.float32), ln2_gain, ln2_bias)

    def next_rows(b):
        res_copy(b).wait()

        @pl.when(b + 1 < n_blocks)
        def _():
            res_copy(b + 1).start()

    @pl.loop(0, n_blocks)
    def _(b):
        serve(BEFORE, b)
        next_rows(b)

        @pl.when(b >= 2)
        def _():
            put_x1(b - 2).wait()

        residual(b, out_proj(b))
        put_x1(b).start()

        @pl.when((b >= LAG) & (b < 2 * LAG - 1))
        def _():
            up_proj(2 * (b - LAG))
            up_proj(2 * (b - LAG) + 1)

        @pl.when(b >= 2 * LAG - 1)
        def _():
            up_proj(b - 1)

    up_proj(n_blocks - 1)
    await_all(xd)
    for b in range(n_blocks - 2, n_blocks):
        put_x1(b).wait()
        put_u(b).wait()
    for copy in caches(NS - 1):
        copy.wait()
    for make, when in sent:
        if when is None:
            make().wait_send()
        else:
            @pl.when(when())
            def _():
                make().wait_send()
    for z_ in range(4):
        wo_y(z_).wait_send()
        wo_x(z_, 1 - y).wait_send()

        @pl.when(z_ != z)
        def _():
            wo_x(z_, y).wait_send()
    pltpu.make_async_copy(whole, whole, wod_s).wait()
    for i, (s, h) in enumerate(CHUNKS):
        pairs = a_all.at[s, h, pl.ds(0, 8)]
        pltpu.make_async_copy(pairs, pairs, ad_s.at[i]).wait()


def front(lens, x, vec, wq, wo, wup, wdn):
    v = pl.BlockSpec(memory_space=pltpu.VMEM)
    sem = lambda n: pltpu.SemaphoreType.DMA((n,))
    one = pltpu.SemaphoreType.DMA
    cache = jax.ShapeDtypeStruct((NS, 2, HD, S), BF)
    rows = lambda n: jax.ShapeDtypeStruct((NS * S // 2, n), BF)
    nc = len(CHUNKS)
    return pl.pallas_call(
        front_kernel,
        out_shape=(cache, cache, rows(D), rows(2 * FF), jax.ShapeDtypeStruct((FF, D), BF)),
        in_specs=[pl.BlockSpec(memory_space=pltpu.SMEM), ANY, v, v, ANY, ANY, ANY],
        out_specs=(ANY,) * 5,
        scratch_shapes=[
            pltpu.VMEM((D, D), BF), pltpu.VMEM((2, D, FF), BF), pltpu.VMEM((NS, 2, 16, 2 * HD, QB), BF), pltpu.VMEM((2, TB, D), BF),
            pltpu.VMEM((2, KA, S), BF), pltpu.VMEM((2, KA, S), BF), pltpu.VMEM((2, HD, S), BF), pltpu.VMEM((2, S, KA), BF),
            pltpu.VMEM((NS, 4, 2 * HD, QB), BF), pltpu.VMEM((8, FF), jnp.float32), pltpu.VMEM((2, TB, D), BF), pltpu.VMEM((2, TB, 2 * FF), BF), pltpu.VMEM((RING, TB, D), BF),
            sem(2), sem(2), sem(2), sem(2), sem(2), sem(6), sem(3), sem(3), sem(4), sem(4), sem(8), sem(8), one, one, sem(nc), sem(nc), sem(6 * nc), sem(3 * nc), sem(3 * nc), sem(nc), sem(nc),
            one, one, sem(UC), sem(UC), sem(UC), sem(UC), sem(UC), sem(UC), sem(UC), sem(UC),
        ],
        compiler_params=pltpu.CompilerParams(collective_id=1, has_side_effects=True, vmem_limit_bytes=63 * 2**20),
        cost_estimate=pl.CostEstimate(flops=10**11, bytes_accessed=10**8, transcendentals=0),
        name="front",
    )(lens, x, vec, wq, wo, wup, wdn)


BR = 128
NB = 3 * S // 2 // BR
Q = BR // 8
CH = BR // 2
SLOTS, S1N = 6, 4


def down_kernel(u_ref, w0_ref, w1_ref, x1_ref, bd_ref, o_ref,
                wd, ub, x1b, pt, acc, s1, r1, sm, rr, rl, fin,
                wsem, usem, xsem, lsem, s1s, r1s, sms, rrs, rls, zs, frs, fls, ys, yr, ds, dr):
    group, me = lax.axis_index("dp"), lax.axis_index("tp")
    z, y, c = me // 4, (me // 2) % 2, me % 2
    dev = lambda z_, y_, c_: (group, z_ * 4 + y_ * 2 + c_)
    partner, ypeer = dev(z, y, 1 - c), dev(z, 1 - y, c)
    right, left = dev((z + 1) % 4, y, c), dev((z + 3) % 4, y, c)

    barrier = pltpu.get_barrier_semaphore()
    for peer in (partner, ypeer, right, left):
        pl.semaphore_signal(barrier, inc=1, device_id=peer, device_id_type=MESH)

    loads = [pltpu.make_async_copy(w, wd.at[pl.ds(i * FF, FF)], wsem.at[i]) for i, w in enumerate((w0_ref, w1_ref))]
    for copy in loads:
        copy.start()

    def u_load(b):
        return pltpu.make_async_copy(u_ref.at[pl.ds(pl.multiple_of(b * BR, BR), BR)], ub.at[b], usem.at[b])

    def x1_load(b):
        rows = pl.ds(pl.multiple_of(b * BR + c * CH + z * Q, Q), Q)
        return pltpu.make_async_copy(x1_ref.at[rows], x1b.at[b], xsem.at[b])

    @pl.loop(0, NB)
    def _(b):
        u_load(b).start()
        x1_load(b).start()

    for copy in loads:
        copy.wait()
    pl.semaphore_wait(barrier, 4)

    per = NB // 3

    def rows_of(b, z_, y_):
        pos = (S // 2) * y_ + BR * (b % per) + CH * c + Q * z_
        return pl.ds(pl.multiple_of((b // per) * S + pos, Q), Q)

    def remote(src, dst, ss, rs, to):
        return pltpu.make_async_remote_copy(src, dst, ss, rs, device_id=to, device_id_type=MESH)

    def swap(b):
        return remote(s1.at[b % S1N], r1.at[b], s1s.at[b % S1N], r1s.at[b], partner)

    def chain(b, n, at, to_right):
        dst, sem = (rr, rrs) if to_right else (rl, rls)
        return remote(sm.at[b, pl.ds(at, n * Q)], dst.at[b, pl.ds(0, n * Q)], sms, sem.at[b], right if to_right else left)

    def go_right(b, k):
        rows = rows_of(b, (z + 4 - k) % 4, y)
        return remote(fin.at[b] if k == 0 else o_ref.at[rows], o_ref.at[rows], zs, frs.at[b * 3 + k], right)

    def go_left(b, k):
        rows = rows_of(b, (z + k) % 4, y)
        return remote(fin.at[b] if k == 0 else o_ref.at[rows], o_ref.at[rows], zs, fls.at[b * 3 + k], left)

    def go_y(b, z_, own=False):
        rows = rows_of(b, z_, y)
        return remote(fin.at[b] if own else o_ref.at[rows], o_ref.at[rows], ys, yr.at[b * 4 + z_], ypeer)

    def go_core(b, z_, y_, own=False):
        rows = rows_of(b, z_, y_)
        return remote(fin.at[b] if own else o_ref.at[rows], o_ref.at[rows], ds, dr, partner)

    f32 = lambda v: v.astype(jnp.float32)

    def multiply(b):
        u_load(b).wait()

        @pl.when(b >= S1N)
        def _():
            swap(b - S1N).wait_send()

        @pl.loop(0, 5)
        def _(j):
            cols = pl.ds(pl.multiple_of(j * 512, 512), 512)
            pt[...] = jnp.dot(ub[b], wd[:, cols], preferred_element_type=jnp.float32)
            acc[b % SLOTS, :, cols] = pt[pl.ds(pl.multiple_of(c * CH, CH), CH)]
            s1[b % S1N, :, cols] = pt[pl.ds(pl.multiple_of((1 - c) * CH, CH), CH)].astype(BF)

        swap(b).start()

    def own(i, n=1):
        return slice(i * Q, (i + n) * Q)

    def pass_sums(b, n):
        a = acc.at[b % SLOTS]
        at = 0 if n >= 3 else 2 * Q
        for to_right in (True, False):
            @pl.when(z == (4 - n if to_right else n - 1))
            def _():
                first = (4 - n) * to_right
                keep = 0 if to_right else n - 1
                rest = first + to_right
                if n < 4:
                    chain(b, n, 0, to_right).wait_recv()
                    got = rr if to_right else rl
                    a[own(first + keep)] += f32(got[b, own(keep)])
                    if n > 1:
                        sm[b, pl.ds(at, (n - 1) * Q)] = (a[own(rest, n - 1)] + f32(got[b, own(to_right, n - 1)])).astype(BF)
                else:
                    sm[b] = a[own(rest, n - 1)].astype(BF)
                if n > 1:
                    chain(b, n - 1, at, to_right).start()

    def stage2(b):
        swap(b).wait_recv()
        acc[b % SLOTS] += f32(r1[b])
        pass_sums(b, 4)

    stage3, stage4 = functools.partial(pass_sums, n=3), functools.partial(pass_sums, n=2)

    def finish(b):
        pass_sums(b, 1)
        a = acc.at[b % SLOTS]
        x1_load(b).wait()
        down = a[pl.ds(pl.multiple_of(z * Q, Q), Q)] + bd_ref[DOWN:DOWN + 1]
        fin[b] = (f32(x1b[b]) + down).astype(BF)
        go_y(b, z, True).start()

        @pl.when(z < 3)
        def _():
            go_right(b, 0).start()

        @pl.when(z > 0)
        def _():
            go_left(b, 0).start()

        go_core(b, z, y, True).start()
        pltpu.make_async_copy(fin.at[b], o_ref.at[rows_of(b, z, y)], lsem).start()

    def relay(b, k):
        @pl.when(z >= k + 1)
        def _():
            go_right(b, k).wait_recv()
            if k < 2:
                @pl.when(z < 3)
                def _():
                    go_right(b, k + 1).start()
            go_y(b, (z + 3 - k) % 4).start()
            go_core(b, (z + 3 - k) % 4, y).start()

        @pl.when(z <= 2 - k)
        def _():
            go_left(b, k).wait_recv()
            if k < 2:
                @pl.when(z > 0)
                def _():
                    go_left(b, k + 1).start()
            go_y(b, (z + 1 + k) % 4).start()
            go_core(b, (z + 1 + k) % 4, y).start()

    def across(b):
        for z_ in range(4):
            go_y(b, z_).wait_recv()
            go_core(b, z_, 1 - y).start()

    stages = (multiply, stage2, stage3, stage4, finish, functools.partial(relay, k=0), functools.partial(relay, k=1), functools.partial(relay, k=2), across)

    @pl.loop(0, NB + len(stages) - 1)
    def _(t):
        for i, stage in enumerate(stages):
            b = t - i

            @pl.when((b >= 0) & (b < NB))
            def _():
                stage(b)

    def drain(sem, n):
        rows = o_ref.at[pl.ds(0, n)]
        pltpu.make_async_copy(rows, rows, sem).wait()

    n = NB * Q
    drain(dr, 8 * n)
    drain(ds, 8 * n)
    drain(ys, 4 * n)
    drain(lsem, n)
    drain(sms, 3 * n)
    ends = (z == 0) | (z == 3)

    @pl.when(ends)
    def _():
        drain(zs, n)

    @pl.when(jnp.logical_not(ends))
    def _():
        drain(zs, 5 * n)

    for b in range(NB - S1N, NB):
        swap(b).wait_send()


def down(u, w0, w1, x1, bd):
    sem = lambda n: pltpu.SemaphoreType.DMA((n,))
    one = pltpu.SemaphoreType.DMA
    return pl.pallas_call(
        down_kernel,
        out_shape=jax.ShapeDtypeStruct((3 * S, D), BF),
        in_specs=[ANY] * 4 + [pl.BlockSpec(memory_space=pltpu.VMEM)],
        out_specs=ANY,
        scratch_shapes=[
            pltpu.VMEM((2 * FF, D), BF), pltpu.VMEM((NB, BR, 2 * FF), BF), pltpu.VMEM((NB, Q, D), BF), pltpu.VMEM((BR, 512), jnp.float32),
            pltpu.VMEM((SLOTS, CH, D), jnp.float32), pltpu.VMEM((S1N, CH, D), BF), pltpu.VMEM((NB, CH, D), BF),
            pltpu.VMEM((NB, 3 * Q, D), BF), pltpu.VMEM((NB, 3 * Q, D), BF), pltpu.VMEM((NB, 3 * Q, D), BF), pltpu.VMEM((NB, Q, D), BF),
            sem(2), sem(NB), sem(NB), one, sem(S1N), sem(NB), one, sem(NB), sem(NB), one, sem(3 * NB), sem(3 * NB), one, sem(4 * NB), one, one,
        ],
        compiler_params=pltpu.CompilerParams(collective_id=0, has_side_effects=True, vmem_limit_bytes=62 * 2**20),
        cost_estimate=pl.CostEstimate(flops=4 * S * D * D, bytes_accessed=4 * D * D, transcendentals=0),
        name="down",
    )(u, w0, w1, x1, bd)


def solution(mesh):
    def local_layer(x_in, seq_lens, ln1_gain, ln1_bias, w_qkv, b_qkv, w_out, b_out, ln2_gain, ln2_bias, w_up, b_up, w_down, b_down):
        f32 = lambda v: v.astype(jnp.float32)
        wq = jnp.transpose(w_qkv, (1, 2, 3, 0)).reshape(6 * HD, D)
        wide = lambda v: jnp.pad(f32(v).reshape(-1), (0, D - v.size))
        vec = jnp.stack([wide(v) for v in (ln1_gain, ln1_bias, b_out, ln2_gain, ln2_bias, b_down, b_up, b_qkv)])
        keys, values, x1, u, down_y = front(seq_lens, x_in, vec, wq, w_out.reshape(2 * HD, D), w_up, w_down)
        x_out = down(u, w_down, down_y, x1, vec).reshape(x_in.shape)
        return x_out, jnp.swapaxes(keys, 2, 3), jnp.swapaxes(values, 2, 3)

    arg_specs = (P("dp", None, None), P("dp"), P(), P(), P(None, None, "tp", None), P(None, "tp", None), P("tp", None, None), P(), P(), P(), P(None, "tp"), P("tp"), P("tp", None), P())
    cache_spec = P("dp", "tp", None, None)
    return jax.shard_map(local_layer, mesh=mesh, in_specs=arg_specs, out_specs=(P("dp", None, None), cache_spec, cache_spec), check_vma=False)
```

```python
import collections
import functools

import jax
import jax.numpy as jnp
from jax import lax
from jax.experimental import pallas as pl
from jax.experimental.pallas import tpu as pltpu
from jax.sharding import PartitionSpec as P

D, S, HD, FF = 2560, 2048, 80, 640
BF = jnp.bfloat16
MESH = pl.DeviceIdType.MESH
ANY = pl.BlockSpec(memory_space=pl.ANY)
NT = (((1,), (1,)), ((), ()))
TN = (((0,), (0,)), ((), ()))
SCALE = HD ** -0.5
LOG2E = 1.4426950408889634


def ln_rows(x, gain, bias):
    centered = x - jnp.mean(x, axis=-1, keepdims=True)
    var = jnp.mean(centered * centered, axis=-1, keepdims=True)
    return (centered * lax.rsqrt(var + 1e-5) * gain + bias).astype(BF)


TB, KA, NS = 256, 96, 3
QB = S // 4
PER_SEQ = S // TB
UC = 4
LAG = 4
RING = LAG + 1
DOWN, UP, QKV = 5, 6, 7
IN_QKV = {"0.6": "w0 v0", "1.1": "v1", "1.4": "w2 u0", "1.7": "b0 b1", "2.2": "h10", "2.3": "v3", "2.4": "h01", "2.5": "u2", "2.7": "p0"}
IN_ATTN = {"0.3": "s0 s1 w1", "1.1": "v2", "1.3": "s2 s3 u1 h00", "2.0": "h11", "2.1": "b2 b3", "2.2": "h02 p1", "2.3": "s4 s5 u3"}
AFTER = ("x h12 p2", "h20 o")
BEFORE = {"0": "r0", "1": "h30 p3", "2": "r1 h21", "3": "h31 b4", "4": "q h22 r2", "5": "h32 h40 b5", "6": "r3 h41", "7": "h50 h42 d", "8": "r4 h51", "9": "h52", "10": "r5"}
CHUNKS = tuple((s, h) for s in range(NS) for h in range(2))


def front_kernel(lens_ref, x_ref, vec_ref, wq_ref, wo_ref, wup_ref, wdn_ref,
                 k_out, v_out, x1_out, u_out, dn_out,
                 wt, wu, a_all, xb, q_s, k_s, v_s, kt, a_st, bu, st1, st2, hid,
                 xsem, csem, osem, lsem, wsem, wos, wor, wol, woy_s, woy_r, wox_s, wox_r, wod_s, wod_r, ay_s, ay_r, as_, ar, al, ad_s, ad_r,
                 b_s, b_r, yu_s, yu_r, yd_s, yd_r, xu_s, xu_r, xd_s, xd_r):
    group, me = lax.axis_index("dp"), lax.axis_index("tp")
    z, y, c = me // 4, (me // 2) % 2, me % 2
    dev = lambda z_, y_, c_: (group, z_ * 4 + y_ * 2 + c_)
    partner, ypeer, across = dev(z, y, 1 - c), dev(z, 1 - y, c), (1 - group, me)
    right, left = dev((z + 1) % 4, y, c), dev((z + 3) % 4, y, c)
    ln1_gain, ln1_bias, b_out, ln2_gain, ln2_bias = (vec_ref[i:i + 1] for i in range(5))
    b_qkv = vec_ref[:, :512].T[:6 * HD, QKV:QKV + 1]
    sent = []

    def remote(src, dst, ss, rs, to):
        return pltpu.make_async_remote_copy(src, dst, ss, rs, device_id=to, device_id_type=MESH)

    def go(make, when=None):
        if when is None:
            make().start()
        else:
            @pl.when(when())
            def _():
                make().start()
        sent.append((make, when))

    place = lambda z_, y_, c_: (z_ * 2 + c_) * 2 + y_
    mine = place(z, y, c)
    half = HD

    def wo_part(z_, y_):
        return wt.at[pl.ds(pl.multiple_of(place(z_, y_, c) * 2 * HD + group * half, 16), half)]

    def wo_whole(z_, y_):
        return wt.at[pl.ds(pl.multiple_of(place(z_, y_, c) * 2 * HD, 32), 2 * HD)]

    def wo_mine():
        return wo_ref.at[pl.ds(pl.multiple_of(group * half, 16), half)]

    def wo_line(k, to_right):
        z_ = (z + 4 - k) % 4 if to_right else (z + k) % 4
        i = k + 3 * (not to_right)
        return remote(wo_mine() if k == 0 else wo_part(z_, y), wo_part(z_, y), wos.at[i], (wor if to_right else wol).at[k], right if to_right else left)

    def wo_y(z_, own=False):
        return remote(wo_mine() if own else wo_part(z_, y), wo_part(z_, y), woy_s.at[z_], woy_r.at[z_], ypeer)

    def wo_x(z_, y_):
        i = z_ + 4 * y_
        return remote(wo_part(z_, y_), wo_part(z_, y_), wox_s.at[i], wox_r.at[i], across)

    def wo_core(z_, y_, own=False):
        return remote(wo_ref if own else wo_whole(z_, y_), wo_whole(z_, y_), wod_s, wod_r, partner)

    def a_y(i):
        s, h = CHUNKS[i]
        return remote(a_st.at[s, 2 * (1 - y) + h], a_all.at[s, h, mine], ay_s.at[i], ay_r.at[i], ypeer)

    def a_line(i, k, to_right):
        s, h = CHUNKS[i]
        z_ = (z + 4 - k) % 4 if to_right else (z + k) % 4
        pair = a_all.at[s, h, pl.ds(place(z_, 0, c), 2)]
        return remote(pair, pair, as_.at[i * 6 + k + 3 * (not to_right)], (ar if to_right else al).at[i * 3 + k], right if to_right else left)

    def a_core(i, z_):
        s, h = CHUNKS[i]
        pair = a_all.at[s, h, pl.ds(place(z_, 0, c), 2)]
        return remote(pair, pair, ad_s.at[i], ad_r.at[i], partner)

    hu, hd = D // 2, FF // 2
    cu, cd = hu // UC, hd // UC

    def up_rows(n):
        return pl.ds(pl.multiple_of(group * hu + n * cu, 32), cu)

    def dn_rows(n):
        return pl.ds(pl.multiple_of(group * hd + n * cd, 16), cd)

    def yu(n):
        return remote(wup_ref.at[up_rows(n)], wu.at[1, up_rows(n)], yu_s.at[n], yu_r.at[n], ypeer)

    def xu(n):
        return remote(wu.at[1, up_rows(n)], wu.at[1, up_rows(n)], xu_s.at[n], xu_r.at[n], across)

    def yd(n):
        return remote(wdn_ref.at[dn_rows(n)], dn_out.at[dn_rows(n)], yd_s.at[n], yd_r.at[n], ypeer)

    def xd(n):
        return remote(dn_out.at[dn_rows(n)], dn_out.at[dn_rows(n)], xd_s.at[n], xd_r.at[n], across)

    def bias_flow():
        return remote(vec_ref.at[:, pl.ds(0, FF)], bu, b_s, b_r, ypeer)

    def hop(line, k, then):
        @pl.when(z >= k + 1)
        def _():
            line(k, True).wait_recv()

        if k < 2:
            go(lambda: line(k + 1, True), lambda: (z >= k + 1) & (z < 3))
        then((z + 3 - k) % 4, z >= k + 1)

        @pl.when(z <= 2 - k)
        def _():
            line(k, False).wait_recv()

        if k < 2:
            go(lambda: line(k + 1, False), lambda: (z <= 2 - k) & (z > 0))
        then((z + 1 + k) % 4, z <= 2 - k)

    def begin(line):
        go(lambda: line(0, True), lambda: z < 3)
        go(lambda: line(0, False), lambda: z > 0)

    def wo_then(z_, when):
        @pl.when(when)
        def _():
            wo_y(z_).start()
            wo_x(z_, y).start()

    def wo_hop(k):
        hop(wo_line, k, wo_then)

    def wo_from_y(k):
        def take(z_):
            wo_y(z_).wait_recv()
            wo_x(z_, 1 - y).start()

        if k == 0:
            take(z)
        else:
            @pl.when(z >= k)
            def _():
                take((z + 4 - k) % 4)

            @pl.when(z <= 3 - k)
            def _():
                take((z + k) % 4)

    def wo_from_x():
        for z_ in range(4):
            @pl.when(z_ != z)
            def _():
                wo_x(z_, y).wait_recv()
                wo_core(z_, y).start()
        for z_ in range(4):
            wo_x(z_, 1 - y).wait_recv()
            wo_core(z_, 1 - y).start()

    def a_send(i):
        go(functools.partial(a_y, i))

    def a_begin(i):
        a_y(i).wait_recv()
        begin(functools.partial(a_line, i))
        a_core(i, z).start()

    def a_hop(i, k):
        def then(z_, when):
            @pl.when(when)
            def _():
                a_core(i, z_).start()
        hop(functools.partial(a_line, i), k, then)

    barrier = pltpu.get_barrier_semaphore()
    peers = (partner, ypeer, across, right, left)
    for p in peers:
        pl.semaphore_signal(barrier, inc=1, device_id=p, device_id_type=MESH)

    def x_copy(g):
        return pltpu.make_async_copy(x_ref.at[g // PER_SEQ, pl.ds(pl.multiple_of((g % PER_SEQ) * TB, TB), TB)], xb.at[g % 2], xsem.at[g % 2])

    x_copy(0).start()
    locals_ = [pltpu.make_async_copy(wo_ref, wo_whole(z, y), wsem.at[0]), pltpu.make_async_copy(wup_ref, wu.at[0], wsem.at[1])]
    for copy in locals_:
        copy.start()
    row = lax.broadcasted_iota(jnp.int32, (KA - HD, S), 0)
    for h in range(2):
        q_s[h, HD:] = jnp.where(row == 0, 1.0, 0.0).astype(BF)
    pl.semaphore_wait(barrier, len(peers))

    begin(wo_line)
    wo_y(z, True).start()
    wo_core(z, y, True).start()
    go(bias_flow)

    x_copy(0).wait()
    x_copy(1).start()
    hid[0] = ln_rows(xb[0].astype(jnp.float32), ln1_gain, ln1_bias)

    def caches(s):
        return [pltpu.make_async_copy(k_s.at[:, pl.ds(0, HD)], k_out.at[s], csem.at[0]), pltpu.make_async_copy(v_s, v_out.at[s], csem.at[1])]

    def send(flow, n):
        go(functools.partial(flow, n))

    def pass_on(flow, onward, n):
        flow(n).wait_recv()
        go(functools.partial(onward, n))

    def await_all(flow):
        for n in range(UC):
            flow(n).wait_recv()

    whole = wt.at[pl.ds(0, D // 2)]

    def wo_ready():
        pltpu.make_async_copy(whole, whole, wod_r).wait()
        bias_flow().wait_recv()
        for copy in locals_:
            copy.wait()

    def a_ready(i):
        s, h = CHUNKS[i]
        pairs = a_all.at[s, h, pl.ds(0, 8)]
        pltpu.make_async_copy(pairs, pairs, ad_r.at[i]).wait()

    def down_over():
        for n in range(UC):
            pass_on(yd, xd, n)

    todo = {
        "w": wo_hop, "v": wo_from_y, "x": wo_from_x, "o": wo_ready,
        "s": a_send, "b": a_begin, "h": a_hop, "r": a_ready,
        "u": functools.partial(send, yu), "p": functools.partial(pass_on, yu, xu), "q": functools.partial(await_all, xu),
        "d": down_over,
    }

    def run(words):
        for w in words.split():
            todo[w[0]](*map(int, w[1:]))

    def serve(table, *key):
        for at, words in table.items():
            @pl.when(functools.reduce(jnp.logical_and, [i == int(n) for i, n in zip(key, at.split("."))]))
            def _():
                run(words)

    @pl.loop(0, NS)
    def _(s):
        n = lens_ref[s]

        @pl.when(s > 0)
        def _():
            for copy in caches(s - 1):
                copy.wait()

        @pl.loop(0, PER_SEQ)
        def _(b):
            g = s * PER_SEQ + b

            @pl.when(g + 1 < NS * PER_SEQ)
            def _():
                x_copy(g + 1).wait()

            @pl.when(g + 2 < NS * PER_SEQ)
            def _():
                x_copy(g + 2).start()

            cols = pl.ds(pl.multiple_of(b * TB, TB), TB)
            keep = b * TB + lax.broadcasted_iota(jnp.int32, (1, TB), 1) < n
            t = lax.dot_general(wq_ref[...], hid[g % 2], NT, preferred_element_type=jnp.float32)
            hid[(g + 1) % 2] = ln_rows(xb[(g + 1) % 2].astype(jnp.float32), ln1_gain, ln1_bias)
            t = (t + b_qkv).astype(BF)
            for i in range(2):
                q_s[i, :HD, cols] = t[i * HD:(i + 1) * HD]
                k_s[i, :HD, cols] = jnp.where(keep, t[(2 + i) * HD:(3 + i) * HD], 0)
                v_s[i, :, cols] = jnp.where(keep, t[(4 + i) * HD:(5 + i) * HD], 0)
            serve(IN_QKV, s, b)

        pos = lax.broadcasted_iota(jnp.int32, (KA - HD, S), 1)
        for i in range(2):
            k_s[i, HD:] = jnp.where((row == 0) & (pos >= n), -1e30, 0.0).astype(BF)
            kt[i] = k_s[i].T
        for copy in caches(s):
            copy.start()

        causal = lax.broadcasted_iota(jnp.int32, (QB, QB), 0) <= lax.broadcasted_iota(jnp.int32, (QB, QB), 1)

        @pl.loop(0, 4)
        def _(t):
            at_q = pl.ds(pl.multiple_of(t * QB, QB), QB)

            def block(h, j, m, l, acc, masked):
                at = pl.ds(pl.multiple_of(j * QB, QB), QB)
                sc = jnp.dot(kt[h, at], q_s[h, :, at_q], preferred_element_type=jnp.float32) * (SCALE * LOG2E)
                if masked:
                    sc = jnp.where(causal, sc, -1e30)
                m_new = jnp.maximum(m, jnp.max(sc, axis=0, keepdims=True))
                p = jnp.exp2(sc - m_new)
                scale = jnp.exp2(m - m_new)
                l = scale * l + jnp.sum(p, axis=0, keepdims=True)
                acc = scale * acc + jnp.dot(v_s[h, :, at], p.astype(BF), preferred_element_type=jnp.float32)
                return m_new, l, acc

            zero = (jnp.full((1, QB), -1e30, jnp.float32), jnp.zeros((1, QB), jnp.float32), jnp.zeros((HD, QB), jnp.float32))
            carry = lax.fori_loop(0, t, lambda j, c: tuple(block(h, j, *c[h], False) for h in range(2)), (zero, zero))
            for h in range(2):
                _, l, acc = block(h, t, *carry[h], True)
                a_st[s, t, h * HD:(h + 1) * HD] = (acc / l).astype(BF)

            @pl.when(t // 2 == y)
            def _():
                a_all[s, t % 2, mine] = a_st[s, t]

            serve(IN_ATTN, s, t)

    per = QB // TB
    n_blocks = NS * 2 * per

    def res_copy(i):
        rows = pl.ds(pl.multiple_of(y * (S // 2) + (i % (2 * per)) * TB, TB), TB)
        return pltpu.make_async_copy(x_ref.at[i // (2 * per), rows], xb.at[i % 2], xsem.at[i % 2])

    def put_x1(i):
        return pltpu.make_async_copy(st1.at[i % 2], x1_out.at[pl.ds(pl.multiple_of(i * TB, TB), TB)], osem.at[i % 2])

    def put_u(i):
        return pltpu.make_async_copy(st2.at[i % 2], u_out.at[pl.ds(pl.multiple_of(i * TB, TB), TB)], lsem.at[i % 2])

    res_copy(0).start()
    for words in AFTER:
        run(words)
    for n in range(UC):
        send(yd, n)

    def up_proj(b):
        @pl.when(b >= 2)
        def _():
            put_u(b - 2).wait()

        for n in range(2):
            up = jnp.dot(hid[b % RING], wu[n], preferred_element_type=jnp.float32) + (bu if n else vec_ref)[UP:UP + 1, :FF]
            st2[b % 2, :, n * FF:(n + 1) * FF] = jnp.maximum(up, 0).astype(BF)
        put_u(b).start()

    def out_proj(b):
        a = a_all[b // (2 * per), (b // per) % 2, :, :, pl.ds(pl.multiple_of((b % per) * TB, TB), TB)].reshape(D, TB)
        return lax.dot_general(a, wt[...], TN, preferred_element_type=jnp.float32)

    def residual(b, o):
        x1 = (xb[b % 2].astype(jnp.float32) + o + b_out).astype(BF)
        st1[b % 2] = x1
        hid[b % RING] = ln_rows(x1.astype(jnp.float32), ln2_gain, ln2_bias)

    def next_rows(b):
        res_copy(b).wait()

        @pl.when(b + 1 < n_blocks)
        def _():
            res_copy(b + 1).start()

    @pl.loop(0, n_blocks)
    def _(b):
        serve(BEFORE, b)
        next_rows(b)

        @pl.when(b >= 2)
        def _():
            put_x1(b - 2).wait()

        residual(b, out_proj(b))
        put_x1(b).start()

        @pl.when((b >= LAG) & (b < 2 * LAG - 1))
        def _():
            up_proj(2 * (b - LAG))
            up_proj(2 * (b - LAG) + 1)

        @pl.when(b >= 2 * LAG - 1)
        def _():
            up_proj(b - 1)

    up_proj(n_blocks - 1)
    await_all(xd)
    for b in range(n_blocks - 2, n_blocks):
        put_x1(b).wait()
        put_u(b).wait()
    for copy in caches(NS - 1):
        copy.wait()
    for make, when in sent:
        if when is None:
            make().wait_send()
        else:
            @pl.when(when())
            def _():
                make().wait_send()
    for z_ in range(4):
        wo_y(z_).wait_send()
        wo_x(z_, 1 - y).wait_send()

        @pl.when(z_ != z)
        def _():
            wo_x(z_, y).wait_send()
    pltpu.make_async_copy(whole, whole, wod_s).wait()
    for i, (s, h) in enumerate(CHUNKS):
        pairs = a_all.at[s, h, pl.ds(0, 8)]
        pltpu.make_async_copy(pairs, pairs, ad_s.at[i]).wait()


def front(lens, x, vec, wq, wo, wup, wdn):
    v = pl.BlockSpec(memory_space=pltpu.VMEM)
    sem = lambda n: pltpu.SemaphoreType.DMA((n,))
    one = pltpu.SemaphoreType.DMA
    cache = jax.ShapeDtypeStruct((NS, 2, HD, S), BF)
    rows = lambda n: jax.ShapeDtypeStruct((NS * S // 2, n), BF)
    nc = len(CHUNKS)
    return pl.pallas_call(
        front_kernel,
        out_shape=(cache, cache, rows(D), rows(2 * FF), jax.ShapeDtypeStruct((FF, D), BF)),
        in_specs=[pl.BlockSpec(memory_space=pltpu.SMEM), ANY, v, v, ANY, ANY, ANY],
        out_specs=(ANY,) * 5,
        scratch_shapes=[
            pltpu.VMEM((D, D), BF), pltpu.VMEM((2, D, FF), BF), pltpu.VMEM((NS, 2, 16, 2 * HD, QB), BF), pltpu.VMEM((2, TB, D), BF),
            pltpu.VMEM((2, KA, S), BF), pltpu.VMEM((2, KA, S), BF), pltpu.VMEM((2, HD, S), BF), pltpu.VMEM((2, S, KA), BF),
            pltpu.VMEM((NS, 4, 2 * HD, QB), BF), pltpu.VMEM((8, FF), jnp.float32), pltpu.VMEM((2, TB, D), BF), pltpu.VMEM((2, TB, 2 * FF), BF), pltpu.VMEM((RING, TB, D), BF),
            sem(2), sem(2), sem(2), sem(2), sem(2), sem(6), sem(3), sem(3), sem(4), sem(4), sem(8), sem(8), one, one, sem(nc), sem(nc), sem(6 * nc), sem(3 * nc), sem(3 * nc), sem(nc), sem(nc),
            one, one, sem(UC), sem(UC), sem(UC), sem(UC), sem(UC), sem(UC), sem(UC), sem(UC),
        ],
        compiler_params=pltpu.CompilerParams(collective_id=1, has_side_effects=True, vmem_limit_bytes=63 * 2**20),
        cost_estimate=pl.CostEstimate(flops=10**11, bytes_accessed=10**8, transcendentals=0),
        name="front",
    )(lens, x, vec, wq, wo, wup, wdn)


BR = 128
NB = 3 * S // 2 // BR
Q = BR // 8
CH = BR // 2
SLOTS, S1N = 6, 4


def down_kernel(u_ref, w0_ref, w1_ref, x1_ref, bd_ref, o_ref,
                wd, ub, x1b, pt, acc, s1, r1, sm, rr, rl, fin,
                wsem, usem, xsem, lsem, s1s, r1s, sms, rrs, rls, zs, frs, fls, ys, yr, ds, dr):
    group, me = lax.axis_index("dp"), lax.axis_index("tp")
    z, y, c = me // 4, (me // 2) % 2, me % 2
    dev = lambda z_, y_, c_: (group, z_ * 4 + y_ * 2 + c_)
    partner, ypeer = dev(z, y, 1 - c), dev(z, 1 - y, c)
    right, left = dev((z + 1) % 4, y, c), dev((z + 3) % 4, y, c)

    barrier = pltpu.get_barrier_semaphore()
    for peer in (partner, ypeer, right, left):
        pl.semaphore_signal(barrier, inc=1, device_id=peer, device_id_type=MESH)

    loads = [pltpu.make_async_copy(w, wd.at[pl.ds(i * FF, FF)], wsem.at[i]) for i, w in enumerate((w0_ref, w1_ref))]
    for copy in loads:
        copy.start()

    def u_load(b):
        return pltpu.make_async_copy(u_ref.at[pl.ds(pl.multiple_of(b * BR, BR), BR)], ub.at[b], usem.at[b])

    def x1_load(b):
        rows = pl.ds(pl.multiple_of(b * BR + c * CH + z * Q, Q), Q)
        return pltpu.make_async_copy(x1_ref.at[rows], x1b.at[b], xsem.at[b])

    @pl.loop(0, NB)
    def _(b):
        u_load(b).start()
        x1_load(b).start()

    for copy in loads:
        copy.wait()
    pl.semaphore_wait(barrier, 4)

    per = NB // 3

    def rows_of(b, z_, y_):
        pos = (S // 2) * y_ + BR * (b % per) + CH * c + Q * z_
        return pl.ds(pl.multiple_of((b // per) * S + pos, Q), Q)

    def remote(src, dst, ss, rs, to):
        return pltpu.make_async_remote_copy(src, dst, ss, rs, device_id=to, device_id_type=MESH)

    def swap(b):
        return remote(s1.at[b % S1N], r1.at[b], s1s.at[b % S1N], r1s.at[b], partner)

    def chain(b, n, at, to_right):
        dst, sem = (rr, rrs) if to_right else (rl, rls)
        return remote(sm.at[b, pl.ds(at, n * Q)], dst.at[b, pl.ds(0, n * Q)], sms, sem.at[b], right if to_right else left)

    def go_right(b, k):
        rows = rows_of(b, (z + 4 - k) % 4, y)
        return remote(fin.at[b] if k == 0 else o_ref.at[rows], o_ref.at[rows], zs, frs.at[b * 3 + k], right)

    def go_left(b, k):
        rows = rows_of(b, (z + k) % 4, y)
        return remote(fin.at[b] if k == 0 else o_ref.at[rows], o_ref.at[rows], zs, fls.at[b * 3 + k], left)

    def go_y(b, z_, own=False):
        rows = rows_of(b, z_, y)
        return remote(fin.at[b] if own else o_ref.at[rows], o_ref.at[rows], ys, yr.at[b * 4 + z_], ypeer)

    def go_core(b, z_, y_, own=False):
        rows = rows_of(b, z_, y_)
        return remote(fin.at[b] if own else o_ref.at[rows], o_ref.at[rows], ds, dr, partner)

    f32 = lambda v: v.astype(jnp.float32)

    def multiply(b):
        u_load(b).wait()

        @pl.when(b >= S1N)
        def _():
            swap(b - S1N).wait_send()

        @pl.loop(0, 5)
        def _(j):
            cols = pl.ds(pl.multiple_of(j * 512, 512), 512)
            pt[...] = jnp.dot(ub[b], wd[:, cols], preferred_element_type=jnp.float32)
            acc[b % SLOTS, :, cols] = pt[pl.ds(pl.multiple_of(c * CH, CH), CH)]
            s1[b % S1N, :, cols] = pt[pl.ds(pl.multiple_of((1 - c) * CH, CH), CH)].astype(BF)

        swap(b).start()

    def own(i, n=1):
        return slice(i * Q, (i + n) * Q)

    def pass_sums(b, n):
        a = acc.at[b % SLOTS]
        at = 0 if n >= 3 else 2 * Q
        for to_right in (True, False):
            @pl.when(z == (4 - n if to_right else n - 1))
            def _():
                first = (4 - n) * to_right
                keep = 0 if to_right else n - 1
                rest = first + to_right
                if n < 4:
                    chain(b, n, 0, to_right).wait_recv()
                    got = rr if to_right else rl
                    a[own(first + keep)] += f32(got[b, own(keep)])
                    if n > 1:
                        sm[b, pl.ds(at, (n - 1) * Q)] = (a[own(rest, n - 1)] + f32(got[b, own(to_right, n - 1)])).astype(BF)
                else:
                    sm[b] = a[own(rest, n - 1)].astype(BF)
                if n > 1:
                    chain(b, n - 1, at, to_right).start()

    def stage2(b):
        swap(b).wait_recv()
        acc[b % SLOTS] += f32(r1[b])
        pass_sums(b, 4)

    stage3, stage4 = functools.partial(pass_sums, n=3), functools.partial(pass_sums, n=2)

    def finish(b):
        pass_sums(b, 1)
        a = acc.at[b % SLOTS]
        x1_load(b).wait()
        down = a[pl.ds(pl.multiple_of(z * Q, Q), Q)] + bd_ref[DOWN:DOWN + 1]
        fin[b] = (f32(x1b[b]) + down).astype(BF)
        go_y(b, z, True).start()

        @pl.when(z < 3)
        def _():
            go_right(b, 0).start()

        @pl.when(z > 0)
        def _():
            go_left(b, 0).start()

        go_core(b, z, y, True).start()
        pltpu.make_async_copy(fin.at[b], o_ref.at[rows_of(b, z, y)], lsem).start()

    def relay(b, k):
        @pl.when(z >= k + 1)
        def _():
            go_right(b, k).wait_recv()
            if k < 2:
                @pl.when(z < 3)
                def _():
                    go_right(b, k + 1).start()
            go_y(b, (z + 3 - k) % 4).start()
            go_core(b, (z + 3 - k) % 4, y).start()

        @pl.when(z <= 2 - k)
        def _():
            go_left(b, k).wait_recv()
            if k < 2:
                @pl.when(z > 0)
                def _():
                    go_left(b, k + 1).start()
            go_y(b, (z + 1 + k) % 4).start()
            go_core(b, (z + 1 + k) % 4, y).start()

    def across(b):
        for z_ in range(4):
            go_y(b, z_).wait_recv()
            go_core(b, z_, 1 - y).start()

    stages = (multiply, stage2, stage3, stage4, finish, functools.partial(relay, k=0), functools.partial(relay, k=1), functools.partial(relay, k=2), across)

    @pl.loop(0, NB + len(stages) - 1)
    def _(t):
        for i, stage in enumerate(stages):
            b = t - i

            @pl.when((b >= 0) & (b < NB))
            def _():
                stage(b)

    def drain(sem, n):
        rows = o_ref.at[pl.ds(0, n)]
        pltpu.make_async_copy(rows, rows, sem).wait()

    n = NB * Q
    drain(dr, 8 * n)
    drain(ds, 8 * n)
    drain(ys, 4 * n)
    drain(lsem, n)
    drain(sms, 3 * n)
    ends = (z == 0) | (z == 3)

    @pl.when(ends)
    def _():
        drain(zs, n)

    @pl.when(jnp.logical_not(ends))
    def _():
        drain(zs, 5 * n)

    for b in range(NB - S1N, NB):
        swap(b).wait_send()


def down(u, w0, w1, x1, bd):
    sem = lambda n: pltpu.SemaphoreType.DMA((n,))
    one = pltpu.SemaphoreType.DMA
    return pl.pallas_call(
        down_kernel,
        out_shape=jax.ShapeDtypeStruct((3 * S, D), BF),
        in_specs=[ANY] * 4 + [pl.BlockSpec(memory_space=pltpu.VMEM)],
        out_specs=ANY,
        scratch_shapes=[
            pltpu.VMEM((2 * FF, D), BF), pltpu.VMEM((NB, BR, 2 * FF), BF), pltpu.VMEM((NB, Q, D), BF), pltpu.VMEM((BR, 512), jnp.float32),
            pltpu.VMEM((SLOTS, CH, D), jnp.float32), pltpu.VMEM((S1N, CH, D), BF), pltpu.VMEM((NB, CH, D), BF),
            pltpu.VMEM((NB, 3 * Q, D), BF), pltpu.VMEM((NB, 3 * Q, D), BF), pltpu.VMEM((NB, 3 * Q, D), BF), pltpu.VMEM((NB, Q, D), BF),
            sem(2), sem(NB), sem(NB), one, sem(S1N), sem(NB), one, sem(NB), sem(NB), one, sem(3 * NB), sem(3 * NB), one, sem(4 * NB), one, one,
        ],
        compiler_params=pltpu.CompilerParams(collective_id=0, has_side_effects=True, vmem_limit_bytes=62 * 2**20),
        cost_estimate=pl.CostEstimate(flops=4 * S * D * D, bytes_accessed=4 * D * D, transcendentals=0),
        name="down",
    )(u, w0, w1, x1, bd)


def solution(mesh):
    def local_layer(x_in, seq_lens, ln1_gain, ln1_bias, w_qkv, b_qkv, w_out, b_out, ln2_gain, ln2_bias, w_up, b_up, w_down, b_down):
        f32 = lambda v: v.astype(jnp.float32)
        wq = jnp.transpose(w_qkv, (1, 2, 3, 0)).reshape(6 * HD, D)
        wide = lambda v: jnp.pad(f32(v).reshape(-1), (0, D - v.size))
        vec = jnp.stack([wide(v) for v in (ln1_gain, ln1_bias, b_out, ln2_gain, ln2_bias, b_down, b_up, b_qkv)])
        keys, values, x1, u, down_y = front(seq_lens, x_in, vec, wq, w_out.reshape(2 * HD, D), w_up, w_down)
        x_out = down(u, w_down, down_y, x1, vec).reshape(x_in.shape)
        return x_out, jnp.swapaxes(keys, 2, 3), jnp.swapaxes(values, 2, 3)

    arg_specs = (P("dp", None, None), P("dp"), P(), P(), P(None, None, "tp", None), P(None, "tp", None), P("tp", None, None), P(), P(), P(), P(None, "tp"), P("tp"), P("tp", None), P())
    cache_spec = P("dp", "tp", None, None)
    return jax.shard_map(local_layer, mesh=mesh, in_specs=arg_specs, out_specs=(P("dp", None, None), cache_spec, cache_spec), check_vma=False)
```
